32 devices in a mesh: probe: 4 (over x, core), fsdp: 8 (over z, y).
Axes of the slice: x: 2, y: 2, z: 4, core: 2. Of those that a mesh axis runs over, the one named last changes fastest.
Arguments:
- hidden: bfloat16 [16384, 2048], P(('probe', 'fsdp')), may hold values from -6 to 6
- norm_gain: bfloat16 [2048], replicated, may hold values from 0.5 to 1.5
- query_weight: bfloat16 [2048, 2048], P('fsdp'), may hold values from -1 to 1
- key_weight: bfloat16 [2048, 512], P('fsdp'), may hold values from -16 to 16
- value_weight: bfloat16 [2048, 512], P('fsdp'), may hold values from -0.125 to 0.125
- output_weight: bfloat16 [2048, 2048], P('fsdp'), may hold values from -0.125 to 0.125
- probe_seed: int32 [4], P('probe'), may hold values from 0 to 1073741823
Outputs:
- curvature_value: float32 [2048, 512], P('fsdp', 'probe')
- curvature_output: float32 [2048, 2048], P('fsdp', 'probe')
The draws below stay inside these ranges and needn't reach their ends.
All inputs are finite; a program needn't handle non-finite values.
Results may differ from the reference program's by a relative error of at most 0.024.
Values may be sent and summed in bfloat16 or wider, within the bound.
A program may use at most 128 MiB of HBM per device.

```python
import jax
import jax.numpy as jnp
from jax import lax

D = 2048
HEADS = 16
KV_HEADS = 4
HEAD_DIM = 128
SEQ = 256
TOK_DEV = 512
QW = 2048
KW = 512
TOKENS = 16384
N_PROBE = 4
N_FSDP = 8


def query_base(key):
    normals = jax.random.normal(jax.random.fold_in(key, 7101), (D, HEADS * HEAD_DIM), jnp.float32)
    return jnp.clip(normals, -6.0, 6.0) * D ** (-0.5)


def draw_query_weight(key, part):
    return query_base(key).astype(jnp.bfloat16)


def draw_key_weight(key, part):
    normals = jax.random.normal(jax.random.fold_in(key, 7102), (D, KV_HEADS * HEAD_DIM), jnp.float32)
    noise_part = jnp.clip(normals, -6.0, 6.0) * D ** (-0.5)
    return noise_part.astype(jnp.bfloat16)


def touch_ends(entries, own_key, least, largest):
    longest = entries.shape.index(max(entries.shape))
    spots = []
    for shift in (0, 1):
        where = [jax.random.randint(jax.random.fold_in(own_key, axis), (), 0, length) for axis, length in enumerate(entries.shape)]
        where[longest] = (where[longest] + shift) % entries.shape[longest]
        spots.append(tuple(where))
    return entries.at[spots[0]].set(least).at[spots[1]].set(largest)


def block_scale(stream_key, extent, split, smallest, largest):
    factor_of = 1.0
    for axis_at, blocks in split:
        draws = jax.random.uniform(jax.random.fold_in(jax.random.fold_in(stream_key, 6), axis_at), (blocks,), jnp.float32, smallest / len(split), largest / len(split))
        factor_of = factor_of * jnp.repeat(jnp.exp(draws), extent[axis_at] // blocks).reshape((-1,) + (1,) * (len(extent) - 1 - axis_at))
    return factor_of


def gaussian(stream_key, shape, scale, bound, split=(), kind=jnp.bfloat16):
    factor_of = block_scale(stream_key, shape, split, -0.22, 0.18) if split else 1.0
    values = jax.random.normal(stream_key, shape, jnp.float32) * scale * factor_of
    return jnp.minimum(jnp.maximum(values, -bound), bound).astype(kind)


def setup_inputs(seed: int = 0) -> dict:
    seeds = jax.random.split(jax.random.key(seed), 8)
    return {
        "hidden": gaussian(seeds[0], (TOKENS, D), 1.0, 6.0, ((0, 32),)),
        "norm_gain": jnp.clip(1.0 + 0.1 * jax.random.normal(seeds[1], (D,), jnp.float32), 0.5, 1.5).astype(jnp.bfloat16),
        "query_weight": draw_query_weight(jax.random.fold_in(seeds[7], 71), 0),
        "key_weight": draw_key_weight(jax.random.fold_in(seeds[7], 71), 0),
        "value_weight": gaussian(seeds[4], (D, KW), D ** -0.5, 0.125, ((0, 8),)),
        "output_weight": gaussian(seeds[5], (QW, D), QW ** -0.5, 0.125, ((0, 8),)),
        "probe_seed": touch_ends(jax.random.randint(seeds[6], (N_PROBE,), 0, 1073741824), jax.random.fold_in(seeds[6], 1), 0, 1073741823).astype(jnp.int32),
    }


norm_eps = 1e-05
rope_base = 500000.0

def sign_table(seed_value, matrix_code, row_total, column_total):
    row_index = lax.broadcasted_iota(jnp.int32, (row_total, column_total), 0)
    column_index = lax.broadcasted_iota(jnp.int32, (row_total, column_total), 1)
    hashed = (row_index * column_total + column_index) * 747796405 + (seed_value * 1664525 + matrix_code * 374761393)
    hashed = hashed ^ lax.shift_right_logical(hashed, jnp.int32(15))
    hashed = hashed * 668265261
    hashed = hashed ^ lax.shift_right_logical(hashed, jnp.int32(13))
    hashed = hashed * 1274126177
    hashed = hashed ^ lax.shift_right_logical(hashed, jnp.int32(16))
    return jnp.where(hashed & 1 == 1, 1.0, -1.0).astype(jnp.bfloat16)

def normalize(rows_in, gain_row):
    values = rows_in.astype(jnp.float32)
    inverse = lax.rsqrt(lax.optimization_barrier(jnp.mean(values * values, axis=1, keepdims=True)) + norm_eps)
    return (values * inverse * gain_row.astype(jnp.float32)[None, :]).astype(jnp.bfloat16)

def rotate(projected, head_count):
    row_count = projected.shape[0]
    columns = projected.shape[1]
    head_size = columns // head_count
    half_dim = head_size // 2
    position = (lax.broadcasted_iota(jnp.int32, (row_count, 1), 0) % SEQ).astype(jnp.float32)
    exponent = lax.broadcasted_iota(jnp.int32, (1, half_dim), 1).astype(jnp.float32) * (-2.0 / head_size)
    frequency = jnp.power(jnp.float32(rope_base), exponent)
    angles = position * frequency
    cosine = jnp.cos(angles)[:, None, :]
    sine_part = jnp.sin(angles)[:, None, :]
    shaped = projected.reshape(row_count, head_count, head_size)
    leading = shaped[:, :, :half_dim]
    trailing = shaped[:, :, half_dim:]
    turned = jnp.concatenate([leading * cosine - trailing * sine_part, trailing * cosine + leading * sine_part], axis=2)
    return turned.reshape(row_count, columns).astype(jnp.bfloat16)

def attend(query_rows, key_rows):
    row_count = query_rows.shape[0]
    key_heads = key_rows.shape[1] // HEAD_DIM
    group_size = query_rows.shape[1] // key_rows.shape[1]
    sequences = row_count // SEQ
    grouped_query = query_rows.reshape(sequences, SEQ, key_heads, group_size, HEAD_DIM).astype(jnp.float32)
    grouped_key = key_rows.reshape(sequences, SEQ, key_heads, HEAD_DIM).astype(jnp.float32)
    scores = jnp.einsum('bqkgd,bskd->bkgqs', grouped_query, grouped_key) * HEAD_DIM ** (-0.5)
    causal_mask = lax.broadcasted_iota(jnp.int32, (SEQ, SEQ), 0) >= lax.broadcasted_iota(jnp.int32, (SEQ, SEQ), 1)
    scores = jnp.where(causal_mask, scores, -1e+30)
    highest = lax.optimization_barrier(jnp.max(scores, axis=4, keepdims=True))
    raised = jnp.exp(scores - highest)
    return (raised / lax.optimization_barrier(jnp.sum(raised, axis=4, keepdims=True))).astype(jnp.bfloat16)

def mix_values(attention, value_rows):
    sequences = attention.shape[0]
    key_heads = attention.shape[1]
    group_size = attention.shape[2]
    grouped_value = value_rows.reshape(sequences, SEQ, key_heads, HEAD_DIM).astype(jnp.float32)
    combined = jnp.einsum('bkgqs,bskd->bqkgd', attention.astype(jnp.float32), grouped_value)
    return combined.reshape(sequences * SEQ, key_heads * group_size * HEAD_DIM)

def spread_back(attention, upstream):
    sequences = attention.shape[0]
    key_heads = attention.shape[1]
    group_size = attention.shape[2]
    grouped_upstream = upstream.reshape(sequences, SEQ, key_heads, group_size, HEAD_DIM).astype(jnp.float32)
    spread = jnp.einsum('bkgqs,bqkgd->bskd', attention.astype(jnp.float32), grouped_upstream)
    return spread.reshape(sequences * SEQ, key_heads * HEAD_DIM)

def device_terms(rows_in, norm_gain, query_weight, key_weight, value_weight, output_weight, seed_value):
    normed = normalize(rows_in, norm_gain)
    query_rows = rotate(jnp.dot(normed, query_weight, preferred_element_type=jnp.float32), HEADS)
    key_rows = rotate(jnp.dot(normed, key_weight, preferred_element_type=jnp.float32), KV_HEADS)
    value_rows = jnp.dot(normed, value_weight, preferred_element_type=jnp.float32).astype(jnp.bfloat16)
    attention = attend(query_rows, key_rows)
    context = mix_values(attention, value_rows).astype(jnp.bfloat16)
    signs_value = sign_table(seed_value, 0, D, KW)
    signs_out = sign_table(seed_value, 1, QW, D)
    tangent_value = (jnp.dot(normed, signs_value, preferred_element_type=jnp.float32) * D ** (-0.5)).astype(jnp.bfloat16)
    tangent_context = mix_values(attention, tangent_value).astype(jnp.bfloat16)
    forward_part = jnp.dot(tangent_context, output_weight, preferred_element_type=jnp.float32)
    probe_part = jnp.dot(context, signs_out, preferred_element_type=jnp.float32) * QW ** (-0.5)
    cotangent = (forward_part + probe_part).astype(jnp.bfloat16)
    back_context = jnp.dot(cotangent, output_weight.T, preferred_element_type=jnp.float32).astype(jnp.bfloat16)
    back_value = spread_back(attention, back_context).astype(jnp.bfloat16)
    term_value = jnp.dot(normed.T, back_value, preferred_element_type=jnp.float32)
    term_out = jnp.dot(context.T, cotangent, preferred_element_type=jnp.float32)
    return (term_value, term_out)

def reference(hidden, norm_gain, query_weight, key_weight, value_weight, output_weight, probe_seed):
    blocks = N_PROBE * N_FSDP

    def one_block(totals, block_index):
        rows_in = lax.dynamic_slice_in_dim(hidden, block_index * TOK_DEV, TOK_DEV, 0)
        seed_value = probe_seed[block_index // N_FSDP]
        term_value, term_out = device_terms(rows_in, norm_gain, query_weight, key_weight, value_weight, output_weight, seed_value)
        rounded_value = lax.optimization_barrier(term_value.astype(jnp.bfloat16))
        rounded_out = lax.optimization_barrier(term_out.astype(jnp.bfloat16))
        return ((totals[0] + rounded_value.astype(jnp.float32), totals[1] + rounded_out.astype(jnp.float32)), None)
    starting = (jnp.zeros((D, KW), jnp.float32), jnp.zeros((QW, D), jnp.float32))
    totals, unused = lax.scan(one_block, starting, jnp.arange(blocks, dtype=jnp.int32))
    return (totals[0], totals[1])
```

```python
import functools
import heapq
import math

import jax
import jax.numpy as jnp
import numpy as np
from jax import lax
from jax.experimental import pallas as pl
from jax.experimental.pallas import tpu as pltpu
from jax.sharding import PartitionSpec as P

HEAD_DIM = 128
SEQ = 256
TILE = 256
MESH = pl.DeviceIdType.MESH
F32 = jnp.float32
BF16 = jnp.bfloat16

norm_eps = 1e-05
rope_base = 500000.0

MIX_A = 747796405
MIX_B = 668265261
MIX_C = 1274126177
MIX_SEED = 1664525
MIX_CODE = 374761393

ROWS_BY_ROWS = (((1,), (1,)), ((), ()))

US_PER_MB_ICI = 21.5
US_PER_MB_PAIR = 1.6
LATENCY_US = 2.0


def wrap32(value):
    value &= 0xFFFFFFFF
    return value - (1 << 32) if value >= (1 << 31) else value


def turn_tables():
    half = HEAD_DIM // 2
    position = np.arange(SEQ, dtype=np.float64)[:, None]
    angles = position * rope_base ** (-2.0 * np.arange(half, dtype=np.float64)[None] / HEAD_DIM)
    cosine, sine = np.cos(angles), np.sin(angles)
    return (
        np.concatenate([cosine, cosine], axis=1).astype(np.float32),
        np.concatenate([-sine, sine], axis=1).astype(np.float32),
    )


def bits_of(size):
    return [1 << place for place in range(size.bit_length() - 1)]


def low_bit(mask):
    return mask & -mask


def flip(index, mask):
    for bit in (1, 2, 4, 8, 16, 32, 64, 128):
        if mask & bit:
            index = index + bit - 2 * bit * lax.rem(lax.div(index, bit), 2)
    return index


def span(start, size):
    return pl.ds(pl.multiple_of(start, size), size)


class Plan:
    def __init__(self):
        self.now = 0.0
        self.arrivals = []
        self.tasks = []
        self.free = {}
        self.count = 0
        self.done = set()

    def post(self, link, us, action):
        start = max(self.now, self.free.get(link, 0.0))
        self.free[link] = start + us
        self.count += 1
        heapq.heappush(self.arrivals, (start + us + LATENCY_US, self.count, action))

    def task(self, name, us, needs, action):
        self.tasks.append((name, us, frozenset(needs), action))

    def run(self):
        while self.arrivals or self.tasks:
            if self.arrivals and self.arrivals[0][0] <= self.now:
                action = heapq.heappop(self.arrivals)[2]
                self.now += action() or 0.0
                continue
            ready = [entry for entry in self.tasks if entry[2] <= self.done]
            if ready:
                entry = ready[0]
                self.tasks.remove(entry)
                entry[3]()
                self.now += entry[1]
                self.done.add(entry[0])
                continue
            self.now = self.arrivals[0][0]


def stream_shapes(shards, rows, sizes, streams):
    shapes, sems = [], []
    for name, _, width, steps in streams:
        held, masks = 2, list(range(shards))
        for step in steps:
            if step == "x":
                held, slots = 1, list(masks)
            else:
                masks = [mask for mask in masks if not mask & step]
                slots = list(masks)
            shapes.append(((len(slots), rows, held * width), slots))
    return shapes


def layout(shards, tokens, width, query_width, key_width, probes):
    rows = width // shards
    q_part, k_part = query_width // probes, key_width // probes
    bits = bits_of(shards)
    near = bits[1:] if len(bits) > 1 else []
    streams = [
        ("a", 0, q_part // 2, ["x"] + bits),
        ("b", q_part, q_part // 2, bits[:1] + ["x"] + near),
        ("v", 0, k_part, near + bits[:1] + ["x"]),
    ]
    vm = lambda shape, kind=BF16: pltpu.VMEM(shape, kind)
    sem = lambda count: pltpu.SemaphoreType.DMA((count,))
    scratch = {
        "w": vm((probes, width, q_part + 2 * k_part)),
        "o": vm((query_width, width)),
        "hid": vm((tokens, width)),
        "normed": vm((tokens, width)),
        "sgn": vm((query_width, width)),
        "att": vm((probes * (tokens // SEQ) * (q_part // HEAD_DIM), SEQ, SEQ)),
        "tv": vm((tokens, key_width)),
        "raw": vm((tokens, q_part + 2 * k_part), F32),
        "cblk": vm((tokens, q_part)),
        "ctxt": vm((query_width, tokens)),
        "tctx": vm((tokens, query_width)),
        "acc": vm((tokens, width), F32),
        "bvt": vm((key_width, tokens)),
        "rxd": vm((shards, rows, 2 * q_part)),
        "rxdv": vm((shards, rows, 2 * k_part)),
        "local": sem(3 * probes + 2),
    }
    for kind in ("w", "x", "d1", "d3", "o", "od", "rd", "rdv"):
        scratch["send_" + kind] = sem(shards)
        scratch["recv_" + kind] = sem(shards)
    shapes = stream_shapes(shards, rows, None, streams)
    at = 0
    slots = {}
    for name, _, _, steps in streams:
        for step in range(len(steps)):
            shape, slot = shapes[at]
            at += 1
            scratch["rx_%s%d" % (name, step)] = vm(shape)
            scratch["send_%s%d" % (name, step)] = sem(shards)
            scratch["recv_%s%d" % (name, step)] = sem(len(slot))
            slots[name, step] = slot
    return scratch, streams, slots


def kernel(sizes, names, streams, slots, seed_ref, gain_ref, cos_ref, sin_ref, hid_in, q_in, k_in,
           v_in, o_in, value_out, output_out, *refs):
    shards, tokens, width, query_width, key_width, probes = sizes
    ref = dict(zip(names, refs))
    w, o, hid, normed, sgn, att = (ref[n] for n in ("w", "o", "hid", "normed", "sgn", "att"))
    tv, raw, cblk, ctxt, tctx, acc, bvt = (
        ref[n] for n in ("tv", "raw", "cblk", "ctxt", "tctx", "acc", "bvt")
    )
    cot = hid
    rows = width // shards
    q_part, k_part = query_width // probes, key_width // probes
    heads = q_part // HEAD_DIM
    sequences = tokens // SEQ
    out_half = width // 2
    bits = bits_of(shards)
    everyone = list(range(1, shards))

    pr = lax.axis_index("probe")
    fs = lax.axis_index("fsdp")
    core = lax.rem(pr, 2)
    block_of = [flip(pr, mask) for mask in range(probes)]
    shard_of = [flip(fs, mask) for mask in range(shards)]
    seed = seed_ref[0]
    plan = Plan()
    sent = []

    pair = {"probe": flip(pr, 1)}
    across = {"probe": flip(pr, 2)}
    along = {bit: {"fsdp": flip(fs, bit)} for bit in bits}

    def link_of(bit):
        return "y" if bit == bits[0] else "z"

    def push(kind, slot, source, target, device, receive_slot=None):
        copy = pltpu.make_async_remote_copy(
            src_ref=source,
            dst_ref=target,
            send_sem=ref["send_" + kind].at[slot],
            recv_sem=ref["recv_" + kind].at[slot if receive_slot is None else receive_slot],
            device_id=device,
            device_id_type=MESH,
        )
        copy.start()
        sent.append(copy)

    def arrived(kind, slot, target):
        pltpu.make_async_remote_copy(
            src_ref=target,
            dst_ref=target,
            send_sem=ref["send_" + kind].at[0],
            recv_sem=ref["recv_" + kind].at[slot],
            device_id=pair,
            device_id_type=MESH,
        ).wait_recv()

    def shard_rows(mask):
        return span(shard_of[mask] * rows, rows)

    def w_at(block, mask):
        return w.at[block, shard_rows(mask), :]

    def o_at(mask, half):
        return o.at[shard_rows(mask), span(half * out_half, out_half)]

    local = []

    def fetch(source, target):
        copy = pltpu.make_async_copy(source, target, ref["local"].at[len(local)])
        copy.start()
        local.append(copy)

    for block in range(probes):
        there = block_of[block]
        own = shard_rows(0)
        fetch(q_in.at[:, span(there * q_part, q_part)], w.at[block, own, 0:q_part])
        fetch(k_in.at[:, span(there * k_part, k_part)], w.at[block, own, q_part : q_part + k_part])
        fetch(
            v_in.at[:, span(there * k_part, k_part)],
            w.at[block, own, q_part + k_part : q_part + 2 * k_part],
        )
    fetch(o_in, o.at[shard_rows(0), :])
    fetch(hid_in, hid)

    barrier = pltpu.get_barrier_semaphore()
    greeted = [pair, across] + [along[bit] for bit in bits]
    for device in greeted:
        pl.semaphore_signal(barrier, inc=1, device_id=device, device_id_type=MESH)
    pl.semaphore_wait(barrier, len(greeted))

    w_mb = rows * (q_part + 2 * k_part) * 2e-6
    o_mb = rows * out_half * 2e-6
    left = {"w": set(everyone), "x": set(everyone), "o": set(everyone)}

    def finish(kind, mask):
        left[kind].discard(mask)
        if not left[kind]:
            plan.done.add("all_" + kind)

    def ici_us(bit, size_mb):
        return size_mb * US_PER_MB_ICI * (2.0 if bit > 2 else 1.0)

    def send_w(mask, bit):
        got = mask ^ bit
        push("w", got, w_at(0, mask), w_at(0, mask), along[bit])
        plan.post(link_of(bit), ici_us(bit, w_mb), lambda: got_w(got))

    far_masks = {mask for mask in everyone if low_bit(mask) > 2}

    def got_w(mask):
        arrived("w", mask, w_at(0, mask))
        for bit in reversed(bits):
            if bit < low_bit(mask):
                send_w(mask, bit)
        push("x", mask, w_at(0, mask), w_at(2, mask), across)
        plan.post("x", w_mb * US_PER_MB_ICI, lambda: got_x(mask))
        push("d1", mask, w_at(0, mask), w_at(1, mask), pair)
        finish("w", mask)
        if mask in far_masks:
            far_masks.discard(mask)
            if not far_masks:
                start_far_o()

    def got_x(mask):
        arrived("x", mask, w_at(2, mask))
        push("d3", mask, w_at(2, mask), w_at(3, mask), pair)
        finish("x", mask)

    def send_o(mask, bit):
        got = mask ^ bit
        push("o", got, o_at(mask, core), o_at(mask, core), along[bit])
        plan.post(link_of(bit), ici_us(bit, o_mb), lambda: got_o(got))

    def got_o(mask):
        arrived("o", mask, o_at(mask, core))
        for bit in reversed(bits):
            if bit < low_bit(mask):
                send_o(mask, bit)
        push("od", mask, o_at(mask, core), o_at(mask, core), pair)
        finish("o", mask)

    def start_far_o():
        for bit in reversed(bits[1:]):
            send_o(0, bit)

    for copy in local[:3]:
        copy.wait()
    for bit in reversed(bits):
        send_w(0, bit)
    for copy in local[3:]:
        copy.wait()
    send_o(0, bits[0])
    if not far_masks:
        start_far_o()

    def normalize():
        gain = gain_ref[...].astype(F32)

        def step(index, carry):
            part = span(index * 16, 16)
            values = hid[part, :].astype(F32)
            inverse = lax.rsqrt(jnp.mean(values * values, axis=1, keepdims=True) + norm_eps)
            normed[part, :] = (values * inverse * gain).astype(BF16)
            return carry

        lax.fori_loop(0, tokens // 16, step, 0)

    def signs(offset, columns, shape):
        spread = (
            lax.broadcasted_iota(jnp.int32, shape, 0) * columns
            + lax.broadcasted_iota(jnp.int32, shape, 1)
        ) * MIX_A

        def at(start):
            mixed = spread + (start * MIX_A + offset)
            mixed = mixed ^ lax.shift_right_logical(mixed, jnp.int32(15))
            mixed = mixed * MIX_B
            mixed = mixed ^ lax.shift_right_logical(mixed, jnp.int32(13))
            mixed = mixed * MIX_C
            mixed = mixed ^ lax.shift_right_logical(mixed, jnp.int32(16))
            return jnp.where((mixed & 1) == 1, 1.0, -1.0).astype(BF16)

        return at

    deep = width // TILE

    def value_signs(column):
        make = signs(seed * MIX_SEED, key_width, (32, TILE))
        per = TILE // 32

        def step(index, carry):
            tile, part = lax.div(index, per), lax.rem(index, per)
            start = index * 32 * key_width + column * TILE
            att[column * deep + tile, span(part * 32, 32), :] = make(start)
            return carry

        lax.fori_loop(0, width // 32, step, 0)

    def tangent():
        for column in range(key_width // TILE):
            table = att[column * deep : (column + 1) * deep].reshape(width, TILE)
            product = jnp.dot(normed[...], table, preferred_element_type=F32)
            tv[:, column * TILE : (column + 1) * TILE] = (product * width ** (-0.5)).astype(BF16)

    sign_parts = 8

    def out_signs(part):
        make = signs(seed * MIX_SEED + MIX_CODE, width, (16, 512))
        depth = query_width // sign_parts

        def step(index, carry):
            row = part * depth + index * 16
            for column in range(0, width, 512):
                sgn[span(row, 16), column : column + 512] = make(row * width + column)
            return carry

        lax.fori_loop(0, depth // 16, step, 0)

    def project(block):
        if block == 1:
            for mask in everyone:
                arrived("d1", mask, w_at(1, mask))
        if block == 3:
            for mask in everyone:
                arrived("d3", mask, w_at(3, mask))

        def step(index, carry):
            part = span(index * TILE, TILE)
            raw[:, part] = jnp.dot(normed[...], w[block, :, part], preferred_element_type=F32)
            return carry

        lax.fori_loop(0, (q_part + 2 * k_part) // TILE, step, 0)

    mask_shape = (SEQ, SEQ)

    def attend(block):
        there = block_of[block]
        seen = lax.broadcasted_iota(jnp.int32, mask_shape, 0) >= lax.broadcasted_iota(
            jnp.int32, mask_shape, 1
        )
        factor = math.log2(math.e) * HEAD_DIM ** (-0.5)

        def step(sequence, carry):
            part = span(sequence * SEQ, SEQ)
            cosine, sine = cos_ref[...], sin_ref[...]

            def turned(low):
                piece = raw[part, low : low + HEAD_DIM]
                other = pltpu.roll(piece, HEAD_DIM // 2, 1)
                return (piece * cosine + other * sine).astype(BF16)

            key = turned(q_part)
            value = raw[part, q_part + k_part : q_part + 2 * k_part].astype(BF16)
            both = jnp.concatenate([value, tv[part, span(there * k_part, k_part)]], axis=1)
            for head in range(heads):
                low = head * HEAD_DIM
                scores = lax.dot_general(
                    turned(low), key, ROWS_BY_ROWS, preferred_element_type=F32
                )
                scores = jnp.where(seen, scores, -1e30)
                raised = jnp.exp2((scores - jnp.max(scores, axis=1, keepdims=True)) * factor)
                share = 1.0 / jnp.sum(raised, axis=1, keepdims=True)
                weight = (raised * share).astype(BF16)
                att[block * sequences * heads + sequence * heads + head] = weight
                mixed = jnp.dot(weight, both, preferred_element_type=F32)
                first = mixed[:, :HEAD_DIM]
                cblk[part, low : low + HEAD_DIM] = first.astype(BF16)
                ctxt[span(there * q_part + low, HEAD_DIM), part] = first.T.astype(BF16)
                tctx[part, span(there * q_part + low, HEAD_DIM)] = mixed[:, HEAD_DIM:].astype(BF16)
            return carry

        lax.fori_loop(0, sequences, step, 0)

    def probe(block):
        there = block_of[block]

        def step(index, carry):
            part = span(index * TILE, TILE)
            product = jnp.dot(
                cblk[...], sgn[span(there * q_part, q_part), part], preferred_element_type=F32
            )
            acc[:, part] = product if block == 0 else acc[:, part] + product
            return carry

        lax.fori_loop(0, width // TILE, step, 0)

    def transpose_normed():
        for copy in sent:
            copy.wait_send()
        sent.clear()

        def step(index, carry):
            part = span(index * 128, 128)
            w[0, part, 0:tokens] = normed[:, part].astype(F32).T.astype(BF16)
            return carry

        lax.fori_loop(0, width // 128, step, 0)

    def forward():
        for mask in everyone:
            arrived("od", mask, o_at(mask, 1 - core))

        def step(index, carry):
            part = span(index * TILE, TILE)
            product = jnp.dot(tctx[...], o[:, part], preferred_element_type=F32)
            cot[:, part] = (product + acc[:, part] * query_width ** (-0.5)).astype(BF16)
            return carry

        lax.fori_loop(0, width // TILE, step, 0)

    def back_context(block):
        def step(index, carry):
            part = span(index * SEQ, SEQ)
            w[2, block * q_part : (block + 1) * q_part, part] = lax.dot_general(
                o[span(block_of[block] * q_part, q_part), :],
                cot[part, :],
                ROWS_BY_ROWS,
                preferred_element_type=F32,
            ).astype(BF16)
            return carry

        lax.fori_loop(0, sequences, step, 0)

    place_of = {0: 0, 2: 1, 1: 2, 3: 3}

    def spread_back(block):
        def step(sequence, carry):
            part = span(sequence * SEQ, SEQ)
            total = jnp.zeros((HEAD_DIM, SEQ), F32)
            for head in range(heads):
                low = block * q_part + head * HEAD_DIM
                total = total + jnp.dot(
                    w[2, low : low + HEAD_DIM, part],
                    att[block * sequences * heads + sequence * heads + head],
                    preferred_element_type=F32,
                )
            low = place_of[block] * HEAD_DIM
            bvt[low : low + HEAD_DIM, part] = total.astype(BF16)
            return carry

        lax.fori_loop(0, sequences, step, 0)

    def add(read_a, read_b, write, wide):
        chunk = max(16, min(rows, 16384 // wide))

        def step(index, carry):
            part = span(index * chunk, chunk)
            write(part, read_a(part).astype(F32) + read_b(part).astype(F32))
            return carry

        lax.fori_loop(0, rows // chunk, step, 0)
        return rows * wide * 1.5e-6

    table = {}
    for name, base, wide, steps in streams:
        table[name] = (base, wide, steps, set(), set())

    def home(name, mask, low, wide):
        part = slice(mask * rows, (mask + 1) * rows)
        if name == "v":
            return w.at[1, part, low : low + wide]
        return sgn.at[part, low : low + wide]

    def ready(name, step, mask):
        base, wide, steps, waiting, landed = table[name]
        act = steps[step]
        held = 1 if "x" in steps[:step] else 2
        kind = "%s%d" % (name, step)
        inbox = ref["rx_" + kind]
        if act == "x":
            slot = slots[name, step].index(mask)
            push(kind, mask, home(name, mask, base + wide, wide), inbox.at[slot], across, slot)
            plan.post("x", rows * wide * 2e-6 * US_PER_MB_ICI, lambda: land(name, step, mask))
            waiting.add((step, mask))
            return 0.0
        if mask & act:
            got = mask ^ act
            slot = slots[name, step].index(got)
            push(kind, mask, home(name, mask, base, held * wide), inbox.at[slot], along[act], slot)
            plan.post(
                link_of(act),
                ici_us(act, rows * held * wide * 2e-6),
                lambda: land(name, step, got),
            )
            return 0.0
        waiting.add((step, mask))
        return combine(name, step, mask)

    def land(name, step, mask):
        table[name][4].add((step, mask))
        return combine(name, step, mask)

    def combine(name, step, mask):
        base, wide, steps, waiting, landed = table[name]
        if (step, mask) not in waiting or (step, mask) not in landed:
            return 0.0
        held = 1 if "x" in steps[: step + 1] else 2
        kind = "%s%d" % (name, step)
        slot = slots[name, step].index(mask)
        inbox = ref["rx_" + kind]
        arrived(kind, slot, inbox.at[slot])
        mine = home(name, mask, base, held * wide)
        last = step + 1 == len(steps)

        def write(part, total):
            if not last:
                mine[part, :] = total.astype(BF16)
            elif name == "v":
                value_out[part, :] = total
            elif name == "a":
                output_out[part, 0:wide] = total
            else:
                output_out[part, wide : 2 * wide] = total

        us = add(lambda p: mine[p, :], lambda p: inbox[slot, p, :], write, held * wide)
        return us if last else us + ready(name, step + 1, mask)

    def out_term(mask):
        left_part = ctxt[shard_rows(mask), :]
        target = slice(mask * rows, (mask + 1) * rows)
        piece = q_part // 2

        def step(index, carry):
            other, half, far = lax.div(index, 4), lax.rem(lax.div(index, 2), 2), lax.rem(index, 2)
            mine_core, mine_far = lax.rem(pr, 2), lax.div(pr, 2)
            block = (mine_far + far - 2 * mine_far * far) * 2 + (
                mine_core + other - 2 * mine_core * other
            )
            columns = span(block * q_part + half * piece, piece)
            sgn[target, span(index * piece, piece)] = jnp.dot(
                left_part, cot[:, columns], preferred_element_type=F32
            ).astype(BF16)
            return carry

        lax.fori_loop(0, width // piece, step, 0)
        push("rd", mask, home("a", mask, 2 * q_part, 2 * q_part), ref["rxd"].at[mask], pair)

        def met():
            arrived("rd", mask, ref["rxd"].at[mask])
            mine = home("a", mask, 0, 2 * q_part)

            def write(part, total):
                mine[part, :] = total.astype(BF16)

            us = add(lambda p: mine[p, :], lambda p: ref["rxd"][mask, p, :], write, 2 * q_part)
            us += ready("b", 0, mask)
            return us + ready("a", 0, mask)

        plan.post("pair", rows * 2 * q_part * 2e-6 * US_PER_MB_PAIR, met)

    def value_term(mask):
        target = slice(mask * rows, (mask + 1) * rows)
        w[1, target, 0:key_width] = lax.dot_general(
            w[0, shard_rows(mask), 0:tokens], bvt[...], ROWS_BY_ROWS, preferred_element_type=F32
        ).astype(BF16)
        push("rdv", mask, home("v", mask, 2 * k_part, 2 * k_part), ref["rxdv"].at[mask], pair)

        def met():
            arrived("rdv", mask, ref["rxdv"].at[mask])
            mine = home("v", mask, 0, 2 * k_part)

            def write(part, total):
                mine[part, :] = total.astype(BF16)

            us = add(lambda p: mine[p, :], lambda p: ref["rxdv"][mask, p, :], write, 2 * k_part)
            return us + ready("v", 0, mask)

        plan.post("pair", rows * 2 * k_part * 2e-6 * US_PER_MB_PAIR, met)

    plan.task("norm", 1.5, (), normalize)
    for column in range(key_width // TILE):
        plan.task("value_signs%d" % column, 1.3, (), functools.partial(value_signs, column))
    sign_names = ["value_signs%d" % column for column in range(key_width // TILE)]
    plan.task("tangent", 1.5, ["norm"] + sign_names, tangent)
    for part in range(sign_parts):
        plan.task("out_signs%d" % part, 1.2, (), functools.partial(out_signs, part))
    sign_names = ["out_signs%d" % part for part in range(sign_parts)]
    before = ["tangent"] + sign_names
    for block in range(probes):
        arrival = "all_w" if block < 2 else "all_x"
        plan.task("project%d" % block, 2.5, before + [arrival], functools.partial(project, block))
        plan.task("attend%d" % block, 4.2, ["project%d" % block], functools.partial(attend, block))
        plan.task("probe%d" % block, 1.7, ["attend%d" % block], functools.partial(probe, block))
        before = ["probe%d" % block]
    plan.task("turn", 1.0, before + ["all_o"], transpose_normed)
    plan.task("forward", 5.0, ["turn"], forward)
    out_order = sorted(range(shards), key=lambda mask: [-(mask & bit) for bit in bits])
    value_order = sorted(range(shards), key=lambda mask: [-(mask & b) for b in bits[1:] + bits[:1]])
    terms = [("out%d" % mask, 0.9, ("forward",), functools.partial(out_term, mask)) for mask in out_order]
    chain = []
    for block in range(probes):
        chain.append(("back%d" % block, 1.5, ("forward",), functools.partial(back_context, block)))
        chain.append(
            ("spread%d" % block, 1.0, ("back%d" % block,), functools.partial(spread_back, block))
        )
    spread_names = ["spread%d" % block for block in range(probes)]
    values = [
        ("value%d" % mask, 0.2, spread_names, functools.partial(value_term, mask))
        for mask in value_order
    ]
    merged, early = [], 2
    merged += terms[:early]
    rest = terms[early:]
    while rest or chain:
        merged += chain[:1]
        merged += rest[:1]
        chain, rest = chain[1:], rest[1:]
    for entry in merged + values:
        plan.task(*entry)
    plan.run()
    for copy in sent:
        copy.wait_send()


def body(hidden, norm_gain, query_weight, key_weight, value_weight, output_weight, probe_seed):
    tokens, width = hidden.shape
    query_width, key_width = query_weight.shape[1], key_weight.shape[1]
    probes, shards = lax.axis_size("probe"), lax.axis_size("fsdp")
    sizes = (shards, tokens, width, query_width, key_width, probes)
    assert probes == 4 and key_width == probes * HEAD_DIM and width == query_width
    scratch, streams, slots = layout(*sizes)
    cosine, sine = turn_tables()
    vmem = pl.BlockSpec(memory_space=pltpu.VMEM)
    anywhere = pl.BlockSpec(memory_space=pl.ANY)
    rows = width // shards
    return pl.pallas_call(
        functools.partial(kernel, sizes, list(scratch), streams, slots),
        in_specs=[pl.BlockSpec(memory_space=pltpu.SMEM)] + [vmem] * 3 + [anywhere] * 5,
        out_specs=[vmem, vmem],
        out_shape=[
            jax.ShapeDtypeStruct((rows, key_width // probes), F32),
            jax.ShapeDtypeStruct((rows, width // probes), F32),
        ],
        scratch_shapes=list(scratch.values()),
        compiler_params=pltpu.CompilerParams(
            collective_id=0, has_side_effects=True, vmem_limit_bytes=67043328
        ),
    )(
        probe_seed,
        norm_gain.reshape(1, width),
        jnp.asarray(cosine),
        jnp.asarray(sine),
        hidden,
        query_weight,
        key_weight,
        value_weight,
        output_weight,
    )


def solution(mesh):
    return jax.shard_map(
        body,
        mesh=mesh,
        in_specs=(
            P(("probe", "fsdp"), None),
            P(),
            P("fsdp", None),
            P("fsdp", None),
            P("fsdp", None),
            P("fsdp", None),
            P("probe"),
        ),
        out_specs=(P("fsdp", "probe"), P("fsdp", "probe")),
        check_vma=False,
    )
```

```python
import functools
import heapq
import math

import jax
import jax.numpy as jnp
import numpy as np
from jax import lax
from jax.experimental import pallas as pl
from jax.experimental.pallas import tpu as pltpu
from jax.sharding import PartitionSpec as P

HEAD_DIM = 128
SEQ = 256
TILE = 256
MESH = pl.DeviceIdType.MESH
F32 = jnp.float32
BF16 = jnp.bfloat16

norm_eps = 1e-05
rope_base = 500000.0

MIX_A = 747796405
MIX_B = 668265261
MIX_C = 1274126177
MIX_SEED = 1664525
MIX_CODE = 374761393

ROWS_BY_ROWS = (((1,), (1,)), ((), ()))

US_PER_MB_ICI = 21.5
US_PER_MB_PAIR = 1.6
LATENCY_US = 2.0
AHEAD_US = 5.0
PARTS = 2


def wrap32(value):
    value &= 0xFFFFFFFF
    return value - (1 << 32) if value >= (1 << 31) else value


def turn_tables():
    half = HEAD_DIM // 2
    position = np.arange(SEQ, dtype=np.float64)[:, None]
    angles = position * rope_base ** (-2.0 * np.arange(half, dtype=np.float64)[None] / HEAD_DIM)
    cosine, sine = np.cos(angles), np.sin(angles)
    return (
        np.concatenate([cosine, cosine], axis=1).astype(np.float32),
        np.concatenate([-sine, sine], axis=1).astype(np.float32),
    )


def bits_of(size):
    return [1 << place for place in range(size.bit_length() - 1)]


def low_bit(mask):
    return mask & -mask


def flip(index, mask):
    for bit in (1, 2, 4, 8, 16, 32, 64, 128):
        if mask & bit:
            index = index + bit - 2 * bit * lax.rem(lax.div(index, bit), 2)
    return index


def span(start, unit, size=None):
    return pl.ds(pl.multiple_of(start, unit), unit if size is None else size)


class Plan:
    def __init__(self):
        self.now = 0.0
        self.arrivals = []
        self.waiting = {}
        self.tasks = []
        self.free = {}
        self.count = 0
        self.done = set()

    def post(self, name, link, us, rank, start, action, slow=1.0):
        self.count += 1
        heap = self.waiting.setdefault(link, [])
        heapq.heappush(heap, (rank, self.count, name, us, slow, start, action))
        self.pump()

    def pump(self):
        for link, heap in self.waiting.items():
            while heap and self.free.get(link, 0.0) <= self.now + AHEAD_US:
                rank, count, name, us, slow, start, action = heapq.heappop(heap)
                begin = max(self.now, self.free.get(link, 0.0))
                self.free[link] = begin + us
                start()
                due = begin + us * slow + LATENCY_US
                heapq.heappush(self.arrivals, (due, count, name, action))

    def task(self, name, us, needs, action):
        self.tasks.append((name, us, frozenset(needs), action))

    def run(self):
        while self.arrivals or self.tasks or any(self.waiting.values()):
            self.pump()
            if self.arrivals and self.arrivals[0][0] <= self.now:
                name, action = heapq.heappop(self.arrivals)[2:]
                with jax.named_scope(name):
                    self.now += action() or 0.0
                continue
            ready = [entry for entry in self.tasks if entry[2] <= self.done]
            if ready:
                entry = ready[0]
                self.tasks.remove(entry)
                with jax.named_scope(entry[0]):
                    entry[3]()
                self.now += entry[1]
                self.done.add(entry[0])
                continue
            times = [self.free[link] - AHEAD_US for link, heap in self.waiting.items() if heap]
            times += [entry[0] for entry in self.arrivals[:1]]
            self.now = max(self.now, min(times)) + 1e-6


def stream_shapes(shards, rows, sizes, streams):
    shapes, sems = [], []
    for name, _, width, steps in streams:
        held, masks = 2, list(range(shards))
        for step in steps:
            if step == "x":
                held, slots = 1, list(masks)
            else:
                masks = [mask for mask in masks if not mask & step]
                slots = list(masks)
            shapes.append(((len(slots), rows, held * width), slots))
    return shapes


def layout(shards, tokens, width, query_width, key_width, probes):
    rows = width // shards
    q_part, k_part = query_width // probes, key_width // probes
    bits = bits_of(shards)
    near = bits[1:] if len(bits) > 1 else []
    streams = [
        ("a", 0, q_part // 2, ["x"] + bits),
        ("b", q_part, q_part // 2, bits[:1] + ["x"] + near),
        ("v", 0, k_part, near + bits[:1] + ["x"]),
    ]
    vm = lambda shape, kind=BF16: pltpu.VMEM(shape, kind)
    sem = lambda count: pltpu.SemaphoreType.DMA((count,))
    scratch = {
        "w": vm((probes, width, q_part + 2 * k_part)),
        "o": vm((query_width, width)),
        "hid": vm((tokens, width)),
        "normed": vm((tokens, width)),
        "sgn": vm((query_width, width)),
        "att": vm((probes * (tokens // SEQ) * (q_part // HEAD_DIM), SEQ, SEQ)),
        "tv": vm((tokens, key_width)),
        "raw": vm((2, tokens, q_part + 2 * k_part), F32),
        "cblk": vm((probes, tokens, q_part)),
        "ctxt": vm((query_width, tokens)),
        "tctx": vm((tokens, query_width)),
        "acc": vm((tokens, width), F32),
        "bvt": vm((key_width, tokens)),
        "rxd": vm((shards, rows, 2 * q_part)),
        "rxdv": vm((shards, rows, 2 * k_part)),
        "local": sem(3 * probes + 2),
    }
    for kind in ("w", "x", "d1", "d3", "f", "fd", "e", "ed", "rd", "rdv"):
        scratch["send_" + kind] = sem(shards * PARTS)
        scratch["recv_" + kind] = sem(shards * PARTS)
    shapes = stream_shapes(shards, rows, None, streams)
    at = 0
    slots = {}
    for name, _, _, steps in streams:
        for step in range(len(steps)):
            shape, slot = shapes[at]
            at += 1
            scratch["rx_%s%d" % (name, step)] = vm(shape)
            scratch["send_%s%d" % (name, step)] = sem(shards)
            scratch["recv_%s%d" % (name, step)] = sem(len(slot))
            slots[name, step] = slot
    return scratch, streams, slots


def kernel(sizes, names, streams, slots, seed_ref, gain_ref, cos_ref, sin_ref, hid_in, q_in, k_in,
           v_in, o_in, value_out, output_out, *refs):
    shards, tokens, width, query_width, key_width, probes = sizes
    ref = dict(zip(names, refs))
    w, o, hid, normed, sgn, att = (ref[n] for n in ("w", "o", "hid", "normed", "sgn", "att"))
    tv, raw, cblk, ctxt, tctx, acc, bvt = (
        ref[n] for n in ("tv", "raw", "cblk", "ctxt", "tctx", "acc", "bvt")
    )
    cot = hid
    rows = width // shards
    q_part, k_part = query_width // probes, key_width // probes
    heads = q_part // HEAD_DIM
    sequences = tokens // SEQ
    out_half = width // 2
    bits = bits_of(shards)
    everyone = list(range(1, shards))

    pr = lax.axis_index("probe")
    fs = lax.axis_index("fsdp")
    core = lax.rem(pr, 2)
    block_of = [flip(pr, mask) for mask in range(probes)]
    shard_of = [flip(fs, mask) for mask in range(shards)]
    seed = seed_ref[0]
    plan = Plan()
    sent = {}

    pair = {"probe": flip(pr, 1)}
    across = {"probe": flip(pr, 2)}
    along = {bit: {"fsdp": flip(fs, bit)} for bit in bits}

    def link_of(bit):
        return "y" if bit == bits[0] else "z"

    def push(kind, slot, source, target, device, receive_slot=None):
        copy = pltpu.make_async_remote_copy(
            src_ref=source,
            dst_ref=target,
            send_sem=ref["send_" + kind].at[slot],
            recv_sem=ref["recv_" + kind].at[slot if receive_slot is None else receive_slot],
            device_id=device,
            device_id_type=MESH,
        )
        copy.start()
        sent.setdefault(kind, []).append(copy)

    def drain(kinds):
        for kind in kinds:
            for copy in sent.pop(kind, []):
                copy.wait_send()

    def arrived(kind, slot, target):
        pltpu.make_async_remote_copy(
            src_ref=target,
            dst_ref=target,
            send_sem=ref["send_" + kind].at[0],
            recv_sem=ref["recv_" + kind].at[slot],
            device_id=pair,
            device_id_type=MESH,
        ).wait_recv()

    part_rows = rows // PARTS

    def shard_rows(mask):
        return span(shard_of[mask] * rows, rows)

    def piece_rows(mask, part):
        return span(shard_of[mask] * rows + part * part_rows, part_rows)

    def w_at(block, mask, part):
        return w.at[block, piece_rows(mask, part), :]

    early_lanes = out_half // 4

    def f_at(half, mask, part):
        lanes = span(half * out_half + early_lanes, early_lanes, out_half - early_lanes)
        return o.at[piece_rows(mask, part), lanes]

    def e_at(half, mask, part):
        return o.at[shard_rows(mask), span(half * out_half, early_lanes)]

    local = []

    def fetch(source, target):
        copy = pltpu.make_async_copy(source, target, ref["local"].at[len(local)])
        copy.start()
        local.append(copy)

    for block in range(probes):
        there = block_of[block]
        own = shard_rows(0)
        fetch(q_in.at[:, span(there * q_part, q_part)], w.at[block, own, 0:q_part])
        fetch(k_in.at[:, span(there * k_part, k_part)], w.at[block, own, q_part : q_part + k_part])
        fetch(
            v_in.at[:, span(there * k_part, k_part)],
            w.at[block, own, q_part + k_part : q_part + 2 * k_part],
        )
        if block == 0:
            fetch(hid_in, hid)
            fetch(o_in, o.at[shard_rows(0), :])

    barrier = pltpu.get_barrier_semaphore()
    greeted = [pair, across] + [along[bit] for bit in bits]
    for device in greeted:
        pl.semaphore_signal(barrier, inc=1, device_id=device, device_id_type=MESH)
    pl.semaphore_wait(barrier, len(greeted))

    left = {}

    def finish(kind, mask, part):
        left[kind].discard((mask, part))
        if not any(key[0] == mask for key in left[kind]):
            plan.done.add("%s%d" % (kind, mask))
        if not left[kind]:
            plan.done.add("all_" + kind)

    def hand_over(kind, mask, part, source, target):
        slot = mask * PARTS + part
        plan.post(
            "%s_%d_%d" % (kind, mask, part),
            "pair",
            size_mb(source) * US_PER_MB_PAIR,
            0,
            lambda: push(kind, slot, source, target, pair),
            lambda: finish(kind, mask, part),
        )

    def size_mb(piece):
        return math.prod(piece.shape) * 2e-6

    def channel(kind, order, rank, place, parts, then):
        pieces = {(mask, part) for mask in everyone for part in range(parts)}
        left[kind] = set(pieces)

        def send(mask, part, bit):
            got = mask ^ bit
            here = place(mask, part)
            plan.post(
                "%s_%d_%d" % (kind, got, part),
                link_of(bit),
                size_mb(here) * US_PER_MB_ICI,
                (0.5 if kind == "e" and bit == bits[0] else rank, order.index(bit)),
                lambda: push(kind, got * PARTS + part, here, here, along[bit]),
                lambda: take(got, part),
                2.0 if bit > 2 else 1.0,
            )

        def onward(mask, part, only=None):
            last = max([order.index(bit) for bit in bits if mask & bit], default=-1)
            for bit in order[last + 1 :]:
                if only is None or bit in only:
                    send(mask, part, bit)

        def take(mask, part):
            arrived(kind, mask * PARTS + part, place(mask, part))
            onward(mask, part)
            then(mask, part)
            finish(kind, mask, part)

        return onward

    left["x"] = {(mask, part) for mask in everyone for part in range(PARTS)}
    for kind in ("d1", "d3", "fd"):
        left[kind] = set(left["x"])
    left["ed"] = {(mask, 0) for mask in everyone}

    first_wave = {(mask, part) for mask in everyone[1::2] for part in range(PARTS)}

    def after_w(mask, part):
        here = w_at(0, mask, part)
        first_wave.discard((mask, part))
        if not first_wave and not second_wave:
            second_wave.append(True)
            for piece in range(PARTS):
                start_f(0, piece, bits[1:])
            start_e(0, 0, bits[1:])

        def got_x():
            arrived("x", mask * PARTS + part, w_at(2, mask, part))
            hand_over("d3", mask, part, w_at(2, mask, part), w_at(3, mask, part))
            finish("x", mask, part)

        plan.post(
            "x_%d_%d" % (mask, part),
            "x",
            size_mb(here) * US_PER_MB_ICI,
            0,
            lambda: push("x", mask * PARTS + part, here, w_at(2, mask, part), across),
            got_x,
        )
        hand_over("d1", mask, part, here, w_at(1, mask, part))

    def after_f(mask, part):
        hand_over("fd", mask, part, f_at(core, mask, part), f_at(core, mask, part))

    def after_e(mask, part):
        hand_over("ed", mask, part, e_at(core, mask, part), e_at(core, mask, part))

    start_w = channel("w", bits[::-1], 0, functools.partial(w_at, 0), PARTS, after_w)
    start_f = channel("f", bits[::-1], 1, functools.partial(f_at, core), PARTS, after_f)
    start_e = channel("e", bits[:1] + bits[:0:-1], 2, functools.partial(e_at, core), 1, after_e)

    second_wave = []
    for copy in local[:3]:
        copy.wait()
    for part in range(PARTS):
        start_w(0, part)
    local[4].wait()
    start_e(0, 0, bits[:1])
    for part in range(PARTS):
        start_f(0, part, bits[:1])

    def normalize():
        local[3].wait()
        gain = gain_ref[...].astype(F32)

        def step(index, carry):
            part = span(index * 16, 16)
            values = hid[part, :].astype(F32)
            inverse = lax.rsqrt(jnp.mean(values * values, axis=1, keepdims=True) + norm_eps)
            normed[part, :] = (values * inverse * gain).astype(BF16)
            return carry

        lax.fori_loop(0, tokens // 16, step, 0)

    def signs(offset, columns, shape):
        spread = (
            lax.broadcasted_iota(jnp.int32, shape, 0) * columns
            + lax.broadcasted_iota(jnp.int32, shape, 1)
        ) * MIX_A

        def at(start):
            mixed = spread + (start * MIX_A + offset)
            mixed = mixed ^ lax.shift_right_logical(mixed, jnp.int32(15))
            mixed = mixed * MIX_B
            mixed = mixed ^ lax.shift_right_logical(mixed, jnp.int32(13))
            mixed = mixed * MIX_C
            mixed = mixed ^ lax.shift_right_logical(mixed, jnp.int32(16))
            return jnp.where((mixed & 1) == 1, 1.0, -1.0).astype(BF16)

        return at

    deep = width // TILE

    def value_signs(column):
        make = signs(seed * MIX_SEED, key_width, (32, TILE))
        per = TILE // 32

        def step(index, carry):
            tile, part = lax.div(index, per), lax.rem(index, per)
            start = index * 32 * key_width + column * TILE
            att[column * deep + tile, span(part * 32, 32), :] = make(start)
            return carry

        lax.fori_loop(0, width // 32, step, 0)

    def tangent():
        for column in range(key_width // TILE):
            table = att[column * deep : (column + 1) * deep].reshape(width, TILE)
            product = jnp.dot(normed[...], table, preferred_element_type=F32)
            tv[:, column * TILE : (column + 1) * TILE] = (product * width ** (-0.5)).astype(BF16)

    sign_parts = 8

    def out_signs(part):
        make = signs(seed * MIX_SEED + MIX_CODE, width, (16, 512))
        depth = query_width // sign_parts

        def step(index, carry):
            row = part * depth + index * 16
            for column in range(0, width, 512):
                sgn[span(row, 16), column : column + 512] = make(row * width + column)
            return carry

        lax.fori_loop(0, depth // 16, step, 0)

    def project(block):
        def step(index, carry):
            part = span(index * TILE, TILE)
            raw[block % 2, :, part] = jnp.dot(
                normed[...], w[block, :, part], preferred_element_type=F32
            )
            return carry

        lax.fori_loop(0, (q_part + 2 * k_part) // TILE, step, 0)

    def bring(block, masks):
        if 0 in masks and block:
            for copy in local[2 + 3 * block : 5 + 3 * block]:
                copy.wait()
        if block % 2:
            for mask in masks:
                for part in range(PARTS if mask else 0):
                    arrived(flags[block], mask * PARTS + part, w_at(block, mask, part))

    def whole_project(block):
        bring(block, range(shards))
        project(block)

    def add_shards(block, masks, first):
        bring(block, masks)
        cut = [normed[:, shard_rows(mask)] for mask in masks]
        left_part = jnp.concatenate(cut, axis=1) if len(cut) > 1 else cut[0]

        def step(index, carry):
            part = span(index * TILE, TILE)
            cut = [w[block, shard_rows(mask), part] for mask in masks]
            right_part = jnp.concatenate(cut, axis=0) if len(cut) > 1 else cut[0]
            product = jnp.dot(left_part, right_part, preferred_element_type=F32)
            raw[block % 2, :, part] = product if first else raw[block % 2, :, part] + product
            return carry

        lax.fori_loop(0, (q_part + 2 * k_part) // TILE, step, 0)

    mask_shape = (SEQ, SEQ)

    def attend(block):
        there = block_of[block]
        seen = lax.broadcasted_iota(jnp.int32, mask_shape, 0) >= lax.broadcasted_iota(
            jnp.int32, mask_shape, 1
        )
        factor = math.log2(math.e) * HEAD_DIM ** (-0.5)

        def step(sequence, carry):
            part = span(sequence * SEQ, SEQ)
            cosine, sine = cos_ref[...], sin_ref[...]

            def turned(low):
                piece = raw[block % 2, part, low : low + HEAD_DIM]
                other = pltpu.roll(piece, HEAD_DIM // 2, 1)
                return (piece * cosine + other * sine).astype(BF16)

            key = turned(q_part)
            value = raw[block % 2, part, q_part + k_part : q_part + 2 * k_part].astype(BF16)
            both = jnp.concatenate([value, tv[part, span(there * k_part, k_part)]], axis=1)
            for head in range(heads):
                low = head * HEAD_DIM
                scores = lax.dot_general(
                    turned(low), key, ROWS_BY_ROWS, preferred_element_type=F32
                )
                scores = jnp.where(seen, scores, -1e30)
                raised = jnp.exp2((scores - jnp.max(scores, axis=1, keepdims=True)) * factor)
                share = 1.0 / jnp.sum(raised, axis=1, keepdims=True)
                weight = (raised * share).astype(BF16)
                att[block * sequences * heads + sequence * heads + head] = weight
                mixed = jnp.dot(weight, both, preferred_element_type=F32)
                first = mixed[:, :HEAD_DIM]
                cblk[block, part, low : low + HEAD_DIM] = first.astype(BF16)
                ctxt[span(there * q_part + low, HEAD_DIM), part] = first.T.astype(BF16)
                tctx[part, span(there * q_part + low, HEAD_DIM)] = mixed[:, HEAD_DIM:].astype(BF16)
            return carry

        lax.fori_loop(0, sequences, step, 0)

    def probe_product(blocks, part):
        left_part = jnp.concatenate([cblk[block] for block in blocks], axis=1)
        cut = [sgn[span(block_of[block] * q_part, q_part), part] for block in blocks]
        return jnp.dot(left_part, jnp.concatenate(cut, axis=0), preferred_element_type=F32)

    def probe(blocks):
        def step(index, carry):
            part = span(index * TILE, TILE)
            product = probe_product(blocks, part)
            acc[:, part] = product if 0 in blocks else acc[:, part] + product
            return carry

        lax.fori_loop(0, width // TILE, step, 0)

    def transpose_normed():
        def step(index, carry):
            part = span(index * 128, 128)
            w[0, part, 0:tokens] = normed[:, part].astype(F32).T.astype(BF16)
            return carry

        lax.fori_loop(0, width // 128, step, 0)

    def forward():
        drain(("w", "x", "d1", "d3"))
        for mask in everyone:
            arrived("ed", mask * PARTS, e_at(1 - core, mask, 0))
            for part in range(PARTS):
                arrived("fd", mask * PARTS + part, f_at(1 - core, mask, part))

        def step(index, carry):
            part = span(index * TILE, TILE)
            total = jnp.dot(tctx[...], o[:, part], preferred_element_type=F32)
            total = total + acc[:, part] * query_width ** (-0.5)
            cot[:, part] = total.astype(BF16)
            return carry

        lax.fori_loop(0, width // TILE, step, 0)

    def back_context(block):
        def step(index, carry):
            part = span(index * SEQ, SEQ)
            w[2, block * q_part : (block + 1) * q_part, part] = lax.dot_general(
                o[span(block_of[block] * q_part, q_part), :],
                cot[part, :],
                ROWS_BY_ROWS,
                preferred_element_type=F32,
            ).astype(BF16)
            return carry

        lax.fori_loop(0, sequences, step, 0)

    place_of = {0: 0, 2: 1, 1: 2, 3: 3}

    def spread_back(block):
        def step(sequence, carry):
            part = span(sequence * SEQ, SEQ)
            total = jnp.zeros((HEAD_DIM, SEQ), F32)
            for head in range(heads):
                low = block * q_part + head * HEAD_DIM
                total = total + jnp.dot(
                    w[2, low : low + HEAD_DIM, part],
                    att[block * sequences * heads + sequence * heads + head],
                    preferred_element_type=F32,
                )
            low = place_of[block] * HEAD_DIM
            bvt[low : low + HEAD_DIM, part] = total.astype(BF16)
            return carry

        lax.fori_loop(0, sequences, step, 0)

    def add(read_a, read_b, write, wide):
        chunk = max(16, min(rows, 16384 // wide))

        def step(index, carry):
            part = span(index * chunk, chunk)
            write(part, read_a(part).astype(F32) + read_b(part).astype(F32))
            return carry

        lax.fori_loop(0, rows // chunk, step, 0)
        return rows * wide * 0.8e-6

    table = {}
    for name, base, wide, steps in streams:
        table[name] = (base, wide, steps, set(), set())

    def home(name, mask, low, wide):
        part = slice(mask * rows, (mask + 1) * rows)
        if name == "v":
            return w.at[1, part, low : low + wide]
        return sgn.at[part, low : low + wide]

    def ready(name, step, mask):
        base, wide, steps, waiting, landed = table[name]
        act = steps[step]
        held = 1 if "x" in steps[:step] else 2
        kind = "%s%d" % (name, step)
        inbox = ref["rx_" + kind]
        def still(got):
            later = steps[step + 1 :]
            return sum(1 for other in later if other == "x" or got & other) + (name == "v")

        if act == "x":
            slot = slots[name, step].index(mask)
            source = home(name, mask, base + wide, wide)
            plan.post(
                "%s_%d" % (kind, mask),
                "x",
                size_mb(source) * US_PER_MB_ICI,
                -still(mask),
                lambda: push(kind, mask, source, inbox.at[slot], across, slot),
                lambda: land(name, step, mask),
            )
            waiting.add((step, mask))
            return 0.0
        if mask & act:
            got = mask ^ act
            slot = slots[name, step].index(got)
            source = home(name, mask, base, held * wide)
            plan.post(
                "%s_%d" % (kind, got),
                link_of(act),
                size_mb(source) * US_PER_MB_ICI,
                -still(got),
                lambda: push(kind, mask, source, inbox.at[slot], along[act], slot),
                lambda: land(name, step, got),
                2.0 if act > 2 else 1.0,
            )
            return 0.0
        waiting.add((step, mask))
        return combine(name, step, mask)

    def land(name, step, mask):
        table[name][4].add((step, mask))
        return combine(name, step, mask)

    def combine(name, step, mask):
        base, wide, steps, waiting, landed = table[name]
        if (step, mask) not in waiting or (step, mask) not in landed:
            return 0.0
        held = 1 if "x" in steps[: step + 1] else 2
        kind = "%s%d" % (name, step)
        slot = slots[name, step].index(mask)
        inbox = ref["rx_" + kind]
        arrived(kind, slot, inbox.at[slot])
        mine = home(name, mask, base, held * wide)
        last = step + 1 == len(steps)

        def write(part, total):
            if not last:
                mine[part, :] = total.astype(BF16)
            elif name == "v":
                value_out[part, :] = total
            elif name == "a":
                output_out[part, 0:wide] = total
            else:
                output_out[part, wide : 2 * wide] = total

        us = add(lambda p: mine[p, :], lambda p: inbox[slot, p, :], write, held * wide)
        return us if last else us + ready(name, step + 1, mask)

    def out_term(masks):
        left_part = jnp.concatenate([ctxt[shard_rows(mask), :] for mask in masks], axis=0)
        piece = q_part // 2

        def step(index, carry):
            other, half = lax.div(index, 2), lax.rem(index, 2)
            for far in range(2):
                block = jnp.where(other == 0, block_of[2 * far], block_of[2 * far + 1])
                columns = span(block * q_part + half * piece, piece)
                product = jnp.dot(left_part, cot[:, columns], preferred_element_type=F32)
                for place, mask in enumerate(masks):
                    sgn[mask * rows : (mask + 1) * rows, span((2 * index + far) * piece, piece)] = (
                        product[place * rows : (place + 1) * rows].astype(BF16)
                    )
            return carry

        lax.fori_loop(0, width // piece // 2, step, 0)

        def meet(mask):
            arrived("rd", mask, ref["rxd"].at[mask])
            mine = home("a", mask, 0, 2 * q_part)

            def write(part, total):
                mine[part, :] = total.astype(BF16)

            us = add(lambda p: mine[p, :], lambda p: ref["rxd"][mask, p, :], write, 2 * q_part)
            us += ready("b", 0, mask)
            return us + ready("a", 0, mask)

        for mask in masks:
            source = home("a", mask, 2 * q_part, 2 * q_part)
            plan.post(
                "rd_%d" % mask,
                "pair",
                size_mb(source) * US_PER_MB_PAIR,
                0,
                functools.partial(push, "rd", mask, source, ref["rxd"].at[mask], pair),
                functools.partial(meet, mask),
            )

    def value_term(mask):
        target = slice(mask * rows, (mask + 1) * rows)
        w[1, target, 0:key_width] = lax.dot_general(
            w[0, shard_rows(mask), 0:tokens], bvt[...], ROWS_BY_ROWS, preferred_element_type=F32
        ).astype(BF16)
        def met():
            arrived("rdv", mask, ref["rxdv"].at[mask])
            mine = home("v", mask, 0, 2 * k_part)

            def write(part, total):
                mine[part, :] = total.astype(BF16)

            us = add(lambda p: mine[p, :], lambda p: ref["rxdv"][mask, p, :], write, 2 * k_part)
            return us + ready("v", 0, mask)

        source = home("v", mask, 2 * k_part, 2 * k_part)
        plan.post(
            "rv_%d" % mask,
            "pair",
            size_mb(source) * US_PER_MB_PAIR,
            0,
            lambda: push("rdv", mask, source, ref["rxdv"].at[mask], pair),
            met,
        )

    columns_v = range(key_width // TILE)
    plan.task("norm", 3.7, (), normalize)
    for column in columns_v:
        plan.task("value_signs%d" % column, 1.3, (), functools.partial(value_signs, column))
    needs = ["norm"] + ["value_signs%d" % column for column in columns_v]
    plan.task("tangent", 1.3, needs, tangent)
    for part in range(sign_parts):
        plan.task("out_signs%d" % part, 1.0, (), functools.partial(out_signs, part))
    sign_names = ["out_signs%d" % part for part in range(sign_parts)]
    if rows % 128 == 0:
        arrival_order = sorted(everyone, key=lambda mask: (bin(mask).count("1"), -low_bit(mask)))
        groups = [[0] + arrival_order[:1]]
        groups += [arrival_order[at : at + 2] for at in range(1, shards - 3, 2)]
        groups += [arrival_order[-2:-1], arrival_order[-1:]]
    else:
        groups = [[]]
    flags = ["w", "d1", "x", "d3"]
    before = {0: ["tangent"], 1: ["tangent"], 2: ["attend0"], 3: ["attend1"]}
    for pair_of in ((0, 1), (2, 3)):
        for block in pair_of:
            for index, group in enumerate(groups):
                name = "shards%d_%d" % (block, index)
                if group:
                    arrivals = ["%s%d" % (flags[block], mask) for mask in group if mask]
                    action = functools.partial(add_shards, block, group, index == 0)
                else:
                    arrivals = ["all_" + flags[block]]
                    action = functools.partial(whole_project, block)
                plan.task(name, 0.25 * len(group) + 0.47, before[block] + arrivals, action)
                before[block] = [name]
            name = "attend%d" % block
            plan.task(name, 2.95, before[block] + ["tangent"], functools.partial(attend, block))
        name = "probe%d" % pair_of[0]
        needs = ["attend%d" % block for block in pair_of] + sign_names
        plan.task(name, 3.8, needs, functools.partial(probe, pair_of))
    needs = ["probe0", "probe2", "all_fd", "all_ed"]
    plan.task("forward", 6.0, needs, forward)
    out_order = sorted(range(shards), key=lambda mask: [-(mask & bit) for bit in bits])
    value_order = sorted(range(shards), key=lambda mask: [-(mask & b) for b in bits[1:] + bits[:1]])
    terms = []
    for at in range(0, shards, 2):
        action = functools.partial(out_term, out_order[at : at + 2])
        terms.append(("out%d" % at, 2.2, ("forward",), action))
    chain = []
    for block in range(probes):
        chain.append(("back%d" % block, 1.5, ("forward",), functools.partial(back_context, block)))
        action = functools.partial(spread_back, block)
        chain.append(("spread%d" % block, 0.5, ("back%d" % block,), action))
    chain.append(("turn", 1.5, ("forward", "all_x"), transpose_normed))
    needs = ["turn"] + ["spread%d" % block for block in range(probes)]
    values = [
        ("value%d" % mask, 0.3, needs, functools.partial(value_term, mask)) for mask in value_order
    ]
    merged = terms[:1]
    rest = terms[1:]
    while rest or chain:
        merged += chain[:3]
        merged += rest[:1]
        chain, rest = chain[3:], rest[1:]
    for entry in merged + values:
        plan.task(*entry)
    plan.run()
    drain(list(sent))


def body(hidden, norm_gain, query_weight, key_weight, value_weight, output_weight, probe_seed):
    tokens, width = hidden.shape
    query_width, key_width = query_weight.shape[1], key_weight.shape[1]
    probes, shards = lax.axis_size("probe"), lax.axis_size("fsdp")
    sizes = (shards, tokens, width, query_width, key_width, probes)
    assert probes == 4 and key_width == probes * HEAD_DIM and width == query_width
    scratch, streams, slots = layout(*sizes)
    cosine, sine = turn_tables()
    vmem = pl.BlockSpec(memory_space=pltpu.VMEM)
    anywhere = pl.BlockSpec(memory_space=pl.ANY)
    rows = width // shards
    return pl.pallas_call(
        functools.partial(kernel, sizes, list(scratch), streams, slots),
        in_specs=[pl.BlockSpec(memory_space=pltpu.SMEM)] + [vmem] * 3 + [anywhere] * 5,
        out_specs=[vmem, vmem],
        out_shape=[
            jax.ShapeDtypeStruct((rows, key_width // probes), F32),
            jax.ShapeDtypeStruct((rows, width // probes), F32),
        ],
        scratch_shapes=list(scratch.values()),
        compiler_params=pltpu.CompilerParams(
            collective_id=0, has_side_effects=True, vmem_limit_bytes=67043328
        ),
    )(
        probe_seed,
        norm_gain.reshape(1, width),
        jnp.asarray(cosine),
        jnp.asarray(sine),
        hidden,
        query_weight,
        key_weight,
        value_weight,
        output_weight,
    )


def solution(mesh):
    return jax.shard_map(
        body,
        mesh=mesh,
        in_specs=(
            P(("probe", "fsdp"), None),
            P(),
            P("fsdp", None),
            P("fsdp", None),
            P("fsdp", None),
            P("fsdp", None),
            P("probe"),
        ),
        out_specs=(P("fsdp", "probe"), P("fsdp", "probe")),
        check_vma=False,
    )
```

```python
import functools
import heapq
import math

import jax
import jax.numpy as jnp
import numpy as np
from jax import lax
from jax.experimental import pallas as pl
from jax.experimental.pallas import tpu as pltpu
from jax.sharding import PartitionSpec as P

HEAD_DIM = 128
SEQ = 256
TILE = 256
MESH = pl.DeviceIdType.MESH
F32 = jnp.float32
BF16 = jnp.bfloat16

norm_eps = 1e-05
rope_base = 500000.0

MIX_A = 747796405
MIX_B = 668265261
MIX_C = 1274126177
MIX_SEED = 1664525
MIX_CODE = 374761393

ROWS_BY_ROWS = (((1,), (1,)), ((), ()))

US_PER_MB_ICI = 21.5
US_PER_MB_PAIR = 1.6
LATENCY_US = 2.0
AHEAD_US = 5.0
FIRST_TERMS = 4
CHAIN_STEP = 8
TERM_STEP = 1
PARTS = 2


def wrap32(value):
    value &= 0xFFFFFFFF
    return value - (1 << 32) if value >= (1 << 31) else value


def turn_tables():
    half = HEAD_DIM // 2
    position = np.arange(SEQ, dtype=np.float64)[:, None]
    angles = position * rope_base ** (-2.0 * np.arange(half, dtype=np.float64)[None] / HEAD_DIM)
    cosine, sine = np.cos(angles), np.sin(angles)
    return (
        np.concatenate([cosine, cosine], axis=1).astype(np.float32),
        np.concatenate([-sine, sine], axis=1).astype(np.float32),
    )


def bits_of(size):
    return [1 << place for place in range(size.bit_length() - 1)]


def low_bit(mask):
    return mask & -mask


def flip(index, mask):
    for bit in (1, 2, 4, 8, 16, 32, 64, 128):
        if mask & bit:
            index = index + bit - 2 * bit * lax.rem(lax.div(index, bit), 2)
    return index


def span(start, unit, size=None):
    return pl.ds(pl.multiple_of(start, unit), unit if size is None else size)


class Plan:
    def __init__(self):
        self.now = 0.0
        self.arrivals = []
        self.waiting = {}
        self.tasks = []
        self.free = {}
        self.count = 0
        self.done = set()

    def post(self, name, link, us, rank, start, action, slow=1.0):
        self.count += 1
        heap = self.waiting.setdefault(link, [])
        heapq.heappush(heap, (rank, self.count, name, us, slow, start, action))
        self.pump()

    def pump(self):
        for link, heap in self.waiting.items():
            while heap and self.free.get(link, 0.0) <= self.now + AHEAD_US:
                rank, count, name, us, slow, start, action = heapq.heappop(heap)
                begin = max(self.now, self.free.get(link, 0.0))
                self.free[link] = begin + us
                start()
                due = begin + us * slow + LATENCY_US
                heapq.heappush(self.arrivals, (due, count, name, action))

    def task(self, name, us, needs, action):
        self.tasks.append((name, us, frozenset(needs), action))

    def run(self):
        while self.arrivals or self.tasks or any(self.waiting.values()):
            self.pump()
            if self.arrivals and self.arrivals[0][0] <= self.now:
                name, action = heapq.heappop(self.arrivals)[2:]
                with jax.named_scope(name):
                    self.now += action() or 0.0
                continue
            ready = [entry for entry in self.tasks if entry[2] <= self.done]
            if ready:
                entry = ready[0]
                self.tasks.remove(entry)
                with jax.named_scope(entry[0]):
                    entry[3]()
                self.now += entry[1]
                self.done.add(entry[0])
                continue
            times = [self.free[link] - AHEAD_US for link, heap in self.waiting.items() if heap]
            times += [entry[0] for entry in self.arrivals[:1]]
            self.now = max(self.now, min(times)) + 1e-6


def stream_shapes(shards, rows, sizes, streams):
    shapes, sems = [], []
    for name, _, width, steps in streams:
        held, masks = 2, list(range(shards))
        for step in steps:
            if step == "x":
                held, slots = 1, list(masks)
            else:
                masks = [mask for mask in masks if not mask & step]
                slots = list(masks)
            shapes.append(((len(slots), rows, held * width), slots))
    return shapes


def layout(shards, tokens, width, query_width, key_width, probes):
    rows = width // shards
    q_part, k_part = query_width // probes, key_width // probes
    bits = bits_of(shards)
    near = bits[1:] if len(bits) > 1 else []
    streams = [
        ("a", 0, q_part // 4, ["x"] + bits),
        ("c", q_part // 2, q_part // 4, near + bits[:1] + ["x"]),
        ("b", q_part, q_part // 2, bits[:1] + ["x"] + near),
        ("v", 0, k_part, ["x"] + bits),
    ]
    vm = lambda shape, kind=BF16: pltpu.VMEM(shape, kind)
    sem = lambda count: pltpu.SemaphoreType.DMA((count,))
    scratch = {
        "w": vm((probes, width, q_part + 2 * k_part)),
        "o": vm((query_width, width)),
        "hid": vm((tokens, width)),
        "normed": vm((tokens, width)),
        "sgn": vm((query_width, width)),
        "att": vm((probes * (tokens // SEQ) * (q_part // HEAD_DIM), SEQ, SEQ)),
        "tv": vm((tokens, key_width)),
        "raw": vm((probes, tokens, q_part + 2 * k_part), F32),
        "ctxt": vm((query_width, tokens)),
        "tctx": vm((tokens, query_width)),
        "acc": vm((tokens, width), F32),
        "bvt": vm((key_width, tokens)),
        "rxd": vm((shards, rows, 2 * q_part)),
        "rxdv": vm((shards, rows, 2 * k_part)),
        "local": sem(3 * probes + 2),
    }
    for kind in ("w", "x", "d1", "d3", "f", "fd", "e", "ed", "rd", "rdv"):
        scratch["send_" + kind] = sem(shards * PARTS)
        scratch["recv_" + kind] = sem(shards * PARTS)
    shapes = stream_shapes(shards, rows, None, streams)
    at = 0
    slots = {}
    for name, _, _, steps in streams:
        for step in range(len(steps)):
            shape, slot = shapes[at]
            at += 1
            scratch["rx_%s%d" % (name, step)] = vm(shape)
            scratch["send_%s%d" % (name, step)] = sem(shards)
            scratch["recv_%s%d" % (name, step)] = sem(len(slot))
            slots[name, step] = slot
    return scratch, streams, slots


def kernel(sizes, names, streams, slots, seed_ref, gain_ref, cos_ref, sin_ref, hid_in, q_in, k_in,
           v_in, o_in, value_out, output_out, *refs):
    shards, tokens, width, query_width, key_width, probes = sizes
    ref = dict(zip(names, refs))
    w, o, hid, normed, sgn, att = (ref[n] for n in ("w", "o", "hid", "normed", "sgn", "att"))
    tv, raw, ctxt, tctx, acc, bvt = (
        ref[n] for n in ("tv", "raw", "ctxt", "tctx", "acc", "bvt")
    )
    context = cot = hid
    rows = width // shards
    q_part, k_part = query_width // probes, key_width // probes
    heads = q_part // HEAD_DIM
    sequences = tokens // SEQ
    out_half = width // 2
    bits = bits_of(shards)
    everyone = list(range(1, shards))

    pr = lax.axis_index("probe")
    fs = lax.axis_index("fsdp")
    core = lax.rem(pr, 2)
    block_of = [flip(pr, mask) for mask in range(probes)]
    shard_of = [flip(fs, mask) for mask in range(shards)]
    seed = seed_ref[0]
    plan = Plan()
    sent = {}

    pair = {"probe": flip(pr, 1)}
    across = {"probe": flip(pr, 2)}
    along = {bit: {"fsdp": flip(fs, bit)} for bit in bits}

    def link_of(bit):
        return "y" if bit == bits[0] else "z"

    def push(kind, slot, source, target, device, receive_slot=None):
        copy = pltpu.make_async_remote_copy(
            src_ref=source,
            dst_ref=target,
            send_sem=ref["send_" + kind].at[slot],
            recv_sem=ref["recv_" + kind].at[slot if receive_slot is None else receive_slot],
            device_id=device,
            device_id_type=MESH,
        )
        copy.start()
        sent.setdefault(kind, []).append(copy)

    def drain(kinds):
        for kind in kinds:
            for copy in sent.pop(kind, []):
                copy.wait_send()

    def arrived(kind, slot, target):
        pltpu.make_async_remote_copy(
            src_ref=target,
            dst_ref=target,
            send_sem=ref["send_" + kind].at[0],
            recv_sem=ref["recv_" + kind].at[slot],
            device_id=pair,
            device_id_type=MESH,
        ).wait_recv()

    part_rows = rows // PARTS

    def shard_rows(mask):
        return span(shard_of[mask] * rows, rows)

    def piece_rows(mask, part):
        return span(shard_of[mask] * rows + part * part_rows, part_rows)

    def w_at(block, mask, part):
        return w.at[block, piece_rows(mask, part), :]

    early_lanes = out_half // 4

    def f_at(half, mask, part):
        lanes = span(half * out_half + early_lanes, early_lanes, out_half - early_lanes)
        return o.at[piece_rows(mask, part), lanes]

    def e_at(half, mask, part):
        return o.at[shard_rows(mask), span(half * out_half, early_lanes)]

    local = []

    def fetch(source, target):
        copy = pltpu.make_async_copy(source, target, ref["local"].at[len(local)])
        copy.start()
        local.append(copy)

    for block in range(probes):
        there = block_of[block]
        own = shard_rows(0)
        fetch(q_in.at[:, span(there * q_part, q_part)], w.at[block, own, 0:q_part])
        fetch(k_in.at[:, span(there * k_part, k_part)], w.at[block, own, q_part : q_part + k_part])
        fetch(
            v_in.at[:, span(there * k_part, k_part)],
            w.at[block, own, q_part + k_part : q_part + 2 * k_part],
        )
        if block == 0:
            fetch(hid_in, hid)
            fetch(o_in, o.at[shard_rows(0), :])

    barrier = pltpu.get_barrier_semaphore()
    greeted = [pair, across] + [along[bit] for bit in bits]
    for device in greeted:
        pl.semaphore_signal(barrier, inc=1, device_id=device, device_id_type=MESH)
    pl.semaphore_wait(barrier, len(greeted))

    left = {}

    def finish(kind, mask, part):
        left[kind].discard((mask, part))
        if not any(key[0] == mask for key in left[kind]):
            plan.done.add("%s%d" % (kind, mask))
        if not left[kind]:
            plan.done.add("all_" + kind)

    def hand_over(kind, mask, part, source, target):
        slot = mask * PARTS + part
        plan.post(
            "%s_%d_%d" % (kind, mask, part),
            "pair",
            size_mb(source) * US_PER_MB_PAIR,
            0,
            lambda: push(kind, slot, source, target, pair),
            lambda: finish(kind, mask, part),
        )

    def size_mb(piece):
        return math.prod(piece.shape) * 2e-6

    def channel(kind, order, rank, place, parts, then):
        pieces = {(mask, part) for mask in everyone for part in range(parts)}
        left[kind] = set(pieces)

        def send(mask, part, bit):
            got = mask ^ bit
            here = place(mask, part)
            plan.post(
                "%s_%d_%d" % (kind, got, part),
                link_of(bit),
                size_mb(here) * US_PER_MB_ICI,
                (0.5 if kind == "e" and bit == bits[0] else rank, order.index(bit)),
                lambda: push(kind, got * PARTS + part, here, here, along[bit]),
                lambda: take(got, part),
                2.0 if bit > 2 else 1.0,
            )

        def onward(mask, part, only=None):
            last = max([order.index(bit) for bit in bits if mask & bit], default=-1)
            for bit in order[last + 1 :]:
                if only is None or bit in only:
                    send(mask, part, bit)

        def take(mask, part):
            arrived(kind, mask * PARTS + part, place(mask, part))
            onward(mask, part)
            then(mask, part)
            finish(kind, mask, part)

        return onward

    left["x"] = {(mask, part) for mask in everyone for part in range(PARTS)}
    for kind in ("d1", "d3", "fd"):
        left[kind] = set(left["x"])
    left["ed"] = {(mask, 0) for mask in everyone}

    first_wave = {(mask, part) for mask in everyone[1::2] for part in range(PARTS)}

    def after_w(mask, part):
        here = w_at(0, mask, part)
        first_wave.discard((mask, part))
        if not first_wave and not second_wave:
            second_wave.append(True)
            for piece in range(PARTS):
                start_f(0, piece)
            start_e(0, 0, bits[1:])

        def got_x():
            arrived("x", mask * PARTS + part, w_at(2, mask, part))
            hand_over("d3", mask, part, w_at(2, mask, part), w_at(3, mask, part))
            finish("x", mask, part)

        plan.post(
            "x_%d_%d" % (mask, part),
            "x",
            size_mb(here) * US_PER_MB_ICI,
            0,
            lambda: push("x", mask * PARTS + part, here, w_at(2, mask, part), across),
            got_x,
        )
        hand_over("d1", mask, part, here, w_at(1, mask, part))

    def after_f(mask, part):
        hand_over("fd", mask, part, f_at(core, mask, part), f_at(core, mask, part))

    def after_e(mask, part):
        hand_over("ed", mask, part, e_at(core, mask, part), e_at(core, mask, part))

    start_w = channel("w", bits[::-1], 0, functools.partial(w_at, 0), PARTS, after_w)
    start_f = channel("f", bits[::-1], 1, functools.partial(f_at, core), PARTS, after_f)
    start_e = channel("e", bits[:1] + bits[:0:-1], 2, functools.partial(e_at, core), 1, after_e)

    second_wave = []
    for copy in local[:3]:
        copy.wait()
    for part in range(PARTS):
        start_w(0, part)
    local[4].wait()
    start_e(0, 0, bits[:1])

    def normalize():
        local[3].wait()
        gain = gain_ref[...].astype(F32)

        def step(index, carry):
            part = span(index * 16, 16)
            values = hid[part, :].astype(F32)
            inverse = lax.rsqrt(jnp.mean(values * values, axis=1, keepdims=True) + norm_eps)
            normed[part, :] = (values * inverse * gain).astype(BF16)
            return carry

        lax.fori_loop(0, tokens // 16, step, 0)

    def signs(offset, columns, shape):
        spread = (
            lax.broadcasted_iota(jnp.int32, shape, 0) * columns
            + lax.broadcasted_iota(jnp.int32, shape, 1)
        ) * MIX_A

        def at(start):
            mixed = spread + (start * MIX_A + offset)
            mixed = mixed ^ lax.shift_right_logical(mixed, jnp.int32(15))
            mixed = mixed * MIX_B
            mixed = mixed ^ lax.shift_right_logical(mixed, jnp.int32(13))
            mixed = mixed * MIX_C
            mixed = mixed ^ lax.shift_right_logical(mixed, jnp.int32(16))
            return jnp.where((mixed & 1) == 1, 1.0, -1.0).astype(BF16)

        return at

    deep = width // TILE

    def value_signs(column):
        make = signs(seed * MIX_SEED, key_width, (32, TILE))
        per = TILE // 32

        def step(index, carry):
            tile, part = lax.div(index, per), lax.rem(index, per)
            start = index * 32 * key_width + column * TILE
            att[column * deep + tile, span(part * 32, 32), :] = make(start)
            return carry

        lax.fori_loop(0, width // 32, step, 0)

    def tangent():
        for column in range(key_width // TILE):
            table = att[column * deep : (column + 1) * deep].reshape(width, TILE)
            product = jnp.dot(normed[...], table, preferred_element_type=F32)
            tv[:, column * TILE : (column + 1) * TILE] = (product * width ** (-0.5)).astype(BF16)

    sign_parts = 8

    def out_signs(part):
        make = signs(seed * MIX_SEED + MIX_CODE, width, (16, 512))
        depth = query_width // sign_parts

        def step(index, carry):
            row = part * depth + index * 16
            for column in range(0, width, 512):
                sgn[span(row, 16), column : column + 512] = make(row * width + column)
            return carry

        lax.fori_loop(0, depth // 16, step, 0)

    def project(block):
        def step(index, carry):
            part = span(index * TILE, TILE)
            raw[block, :, part] = jnp.dot(
                normed[...], w[block, :, part], preferred_element_type=F32
            )
            return carry

        lax.fori_loop(0, (q_part + 2 * k_part) // TILE, step, 0)

    def bring(block, masks):
        if 0 in masks and block:
            for copy in local[2 + 3 * block : 5 + 3 * block]:
                copy.wait()
        if block % 2:
            for mask in masks:
                for part in range(PARTS if mask else 0):
                    arrived(flags[block], mask * PARTS + part, w_at(block, mask, part))

    def whole_project(block):
        bring(block, range(shards))
        project(block)

    def add_shards(block, masks, first):
        bring(block, masks)
        cut = [normed[:, shard_rows(mask)] for mask in masks]
        left_part = jnp.concatenate(cut, axis=1) if len(cut) > 1 else cut[0]

        def step(index, carry):
            part = span(index * TILE, TILE)
            cut = [w[block, shard_rows(mask), part] for mask in masks]
            right_part = jnp.concatenate(cut, axis=0) if len(cut) > 1 else cut[0]
            product = jnp.dot(left_part, right_part, preferred_element_type=F32)
            raw[block, :, part] = product if first else raw[block, :, part] + product
            return carry

        lax.fori_loop(0, (q_part + 2 * k_part) // TILE, step, 0)

    mask_shape = (SEQ, SEQ)

    def attend(block):
        there = block_of[block]
        seen = lax.broadcasted_iota(jnp.int32, mask_shape, 0) >= lax.broadcasted_iota(
            jnp.int32, mask_shape, 1
        )
        factor = math.log2(math.e) * HEAD_DIM ** (-0.5)

        def step(sequence, carry):
            part = span(sequence * SEQ, SEQ)
            cosine, sine = cos_ref[...], sin_ref[...]

            def turned(low):
                piece = raw[block, part, low : low + HEAD_DIM]
                other = pltpu.roll(piece, HEAD_DIM // 2, 1)
                return (piece * cosine + other * sine).astype(BF16)

            key = turned(q_part)
            value = raw[block, part, q_part + k_part : q_part + 2 * k_part].astype(BF16)
            both = jnp.concatenate([value, tv[part, span(there * k_part, k_part)]], axis=1)
            for head in range(heads):
                low = head * HEAD_DIM
                scores = lax.dot_general(
                    turned(low), key, ROWS_BY_ROWS, preferred_element_type=F32
                )
                scores = jnp.where(seen, scores, -1e30)
                raised = jnp.exp2((scores - jnp.max(scores, axis=1, keepdims=True)) * factor)
                share = 1.0 / jnp.sum(raised, axis=1, keepdims=True)
                weight = (raised * share).astype(BF16)
                att[block * sequences * heads + sequence * heads + head] = weight
                mixed = jnp.dot(weight, both, preferred_element_type=F32)
                first = mixed[:, :HEAD_DIM]
                context[part, block * q_part + low : block * q_part + low + HEAD_DIM] = first.astype(BF16)
                ctxt[span(there * q_part + low, HEAD_DIM), part] = first.T.astype(BF16)
                tctx[part, span(there * q_part + low, HEAD_DIM)] = mixed[:, HEAD_DIM:].astype(BF16)
            return carry

        lax.fori_loop(0, sequences, step, 0)

    def probe_product(blocks, part):
        left_part = context[:, blocks[0] * q_part : (blocks[-1] + 1) * q_part]
        cut = [sgn[span(block_of[block] * q_part, q_part), part] for block in blocks]
        return jnp.dot(left_part, jnp.concatenate(cut, axis=0), preferred_element_type=F32)

    def probe(blocks):
        def step(index, carry):
            part = span(index * TILE, TILE)
            product = probe_product(blocks, part)
            acc[:, part] = product if 0 in blocks else acc[:, part] + product
            return carry

        lax.fori_loop(0, width // TILE, step, 0)

    def transpose_normed():
        def step(index, carry):
            part = span(index * 128, 128)
            w[1, part, 0:tokens] = normed[:, part].astype(F32).T.astype(BF16)
            return carry

        lax.fori_loop(0, width // 128, step, 0)

    def forward(half):
        if half:
            drain(("w", "x", "d1", "d3"))
        for mask in everyone if half else ():
            arrived("ed", mask * PARTS, e_at(1 - core, mask, 0))
            for part in range(PARTS):
                arrived("fd", mask * PARTS + part, f_at(1 - core, mask, part))

        piece = q_part // 2

        def step(index, carry):
            part = span((2 * index + half) * piece, piece)
            total = jnp.dot(tctx[...], o[:, part], preferred_element_type=F32)
            total = total + acc[:, part] * query_width ** (-0.5)
            cot[:, part] = total.astype(BF16)
            return carry

        lax.fori_loop(0, probes, step, 0)

    def back_context(block):
        def step(index, carry):
            part = span(index * SEQ, SEQ)
            w[2, block * q_part : (block + 1) * q_part, part] = lax.dot_general(
                o[span(block_of[block] * q_part, q_part), :],
                cot[part, :],
                ROWS_BY_ROWS,
                preferred_element_type=F32,
            ).astype(BF16)
            return carry

        lax.fori_loop(0, sequences, step, 0)

    place_of = {0: 0, 1: 1, 2: 2, 3: 3}

    def spread_back(block):
        def step(sequence, carry):
            part = span(sequence * SEQ, SEQ)
            total = jnp.zeros((HEAD_DIM, SEQ), F32)
            for head in range(heads):
                low = block * q_part + head * HEAD_DIM
                total = total + jnp.dot(
                    w[2, low : low + HEAD_DIM, part],
                    att[block * sequences * heads + sequence * heads + head],
                    preferred_element_type=F32,
                )
            low = place_of[block] * HEAD_DIM
            bvt[low : low + HEAD_DIM, part] = total.astype(BF16)
            return carry

        lax.fori_loop(0, sequences, step, 0)

    def add(read_a, read_b, write, wide):
        chunk = max(16, min(rows, 16384 // wide))

        def step(index, carry):
            part = span(index * chunk, chunk)
            write(part, read_a(part).astype(F32) + read_b(part).astype(F32))
            return carry

        lax.fori_loop(0, rows // chunk, step, 0)
        return rows * wide * 0.8e-6

    table = {}
    for name, base, wide, steps in streams:
        table[name] = (base, wide, steps, set(), set())

    def home(name, mask, low, wide):
        part = slice(mask * rows, (mask + 1) * rows)
        if name == "v":
            return w.at[0, part, low : low + wide]
        return sgn.at[part, low : low + wide]

    def ready(name, step, mask):
        base, wide, steps, waiting, landed = table[name]
        act = steps[step]
        held = 1 if "x" in steps[:step] else 2
        kind = "%s%d" % (name, step)
        inbox = ref["rx_" + kind]
        def still(got):
            later = steps[step + 1 :]
            return sum(1 for other in later if other == "x" or got & other) + (name == "v")

        if act == "x":
            slot = slots[name, step].index(mask)
            source = home(name, mask, base + (2 * wide if name == "v" else wide), wide)
            plan.post(
                "%s_%d" % (kind, mask),
                "x",
                size_mb(source) * US_PER_MB_ICI,
                -still(mask),
                lambda: push(kind, mask, source, inbox.at[slot], across, slot),
                lambda: land(name, step, mask),
            )
            if name != "v":
                waiting.add((step, mask))
            return 0.0
        if mask & act:
            got = mask ^ act
            slot = slots[name, step].index(got)
            source = home(name, mask, base, held * wide)
            plan.post(
                "%s_%d" % (kind, got),
                link_of(act),
                size_mb(source) * US_PER_MB_ICI,
                -still(got),
                lambda: push(kind, mask, source, inbox.at[slot], along[act], slot),
                lambda: land(name, step, got),
                2.0 if act > 2 else 1.0,
            )
            return 0.0
        waiting.add((step, mask))
        return combine(name, step, mask)

    def land(name, step, mask):
        table[name][4].add((step, mask))
        return combine(name, step, mask)

    def combine(name, step, mask):
        base, wide, steps, waiting, landed = table[name]
        if (step, mask) not in waiting or (step, mask) not in landed:
            return 0.0
        held = 1 if "x" in steps[: step + 1] else 2
        kind = "%s%d" % (name, step)
        slot = slots[name, step].index(mask)
        inbox = ref["rx_" + kind]
        arrived(kind, slot, inbox.at[slot])
        mine = home(name, mask, base, held * wide)
        last = step + 1 == len(steps)

        def write(part, total):
            if not last:
                mine[part, :] = total.astype(BF16)
            elif name == "v":
                value_out[part, :] = total
            else:
                output_out[part, base // 2 : base // 2 + wide] = total

        us = add(lambda p: mine[p, :], lambda p: inbox[slot, p, :], write, held * wide)
        return us if last else us + ready(name, step + 1, mask)

    def out_term(masks, half):
        left_part = jnp.concatenate([ctxt[shard_rows(mask), :] for mask in masks], axis=0)
        piece, quarter = q_part // 2, q_part // 4

        def step(other, carry):
            for far in range(2):
                block = jnp.where(other == 0, block_of[2 * far], block_of[2 * far + 1])
                columns = span(block * q_part + half * piece, piece)
                product = jnp.dot(left_part, cot[:, columns], preferred_element_type=F32)
                for place, mask in enumerate(masks):
                    target = slice(mask * rows, (mask + 1) * rows)
                    part = product[place * rows : (place + 1) * rows].astype(BF16)
                    if half:
                        sgn[target, span(other * 2 * q_part + q_part + far * piece, piece)] = part
                    else:
                        low = other * 2 * q_part + far * quarter
                        sgn[target, span(low, quarter)] = part[:, :quarter]
                        sgn[target, span(low + 2 * quarter, quarter)] = part[:, quarter:]
            return carry

        lax.fori_loop(0, 2, step, 0)
        low = half * q_part

        def meet(mask):
            inbox = ref["rxd"].at[mask, :, low : low + q_part]
            arrived("rd", mask * PARTS + half, inbox)
            mine = home("a", mask, low, q_part)

            def write(part, total):
                mine[part, :] = total.astype(BF16)

            us = add(lambda p: mine[p, :], lambda p: inbox[p, :], write, q_part)
            for name in ("b",) if half else ("c", "a"):
                us += ready(name, 0, mask)
            return us

        for mask in masks:
            source = home("a", mask, 2 * q_part + low, q_part)
            inbox = ref["rxd"].at[mask, :, low : low + q_part]
            slot = mask * PARTS + half
            plan.post(
                "rd%d_%d" % (half, mask),
                "pair",
                size_mb(source) * US_PER_MB_PAIR,
                0,
                functools.partial(push, "rd", slot, source, inbox, pair),
                functools.partial(meet, mask),
            )

    def value_term(masks, group):
        low = group * 2 * k_part
        left_part = jnp.concatenate([w[1, shard_rows(mask), 0:tokens] for mask in masks], axis=0)
        product = lax.dot_general(
            left_part, bvt[low : low + 2 * k_part, :], ROWS_BY_ROWS, preferred_element_type=F32
        ).astype(BF16)
        for place, mask in enumerate(masks):
            target = slice(mask * rows, (mask + 1) * rows)
            w[0, target, low : low + 2 * k_part] = product[place * rows : (place + 1) * rows]

        def met(mask):
            inbox = ref["rxdv"].at[mask, :, group * k_part : (group + 1) * k_part]
            arrived("rdv", mask * PARTS + group, inbox)
            mine = home("v", mask, low, k_part)

            def write(part, total):
                mine[part, :] = total.astype(BF16)

            us = add(lambda p: mine[p, :], lambda p: inbox[p, :], write, k_part)
            if group:
                return us + ready("v", 0, mask)
            table["v"][3].add((0, mask))
            return us + combine("v", 0, mask)

        for mask in masks:
            source = home("v", mask, low + k_part, k_part)
            inbox = ref["rxdv"].at[mask, :, group * k_part : (group + 1) * k_part]
            plan.post(
                "rv%d_%d" % (group, mask),
                "pair",
                size_mb(source) * US_PER_MB_PAIR,
                0,
                functools.partial(
                    push, "rdv", mask * PARTS + group, source, inbox, pair
                ),
                functools.partial(met, mask),
            )

    columns_v = range(key_width // TILE)
    plan.task("norm", 3.7, (), normalize)
    for column in columns_v:
        plan.task("value_signs%d" % column, 1.3, (), functools.partial(value_signs, column))
    needs = ["norm"] + ["value_signs%d" % column for column in columns_v]
    plan.task("tangent", 1.3, needs, tangent)
    for part in range(sign_parts):
        plan.task("out_signs%d" % part, 1.0, (), functools.partial(out_signs, part))
    sign_names = ["out_signs%d" % part for part in range(sign_parts)]
    if rows % 128 == 0:
        arrival_order = sorted(everyone, key=lambda mask: (bin(mask).count("1"), -low_bit(mask)))
        groups = [[0] + arrival_order[:1]]
        groups += [arrival_order[at : at + 2] for at in range(1, shards - 3, 2)]
        groups += [arrival_order[-2:-1], arrival_order[-1:]]
    else:
        groups = [[]]
    flags = ["w", "d1", "x", "d3"]
    before = {block: ["norm"] for block in range(probes)}
    for pair_of in ((0, 1), (2, 3)):
        for block in pair_of:
            for index, group in enumerate(groups):
                name = "shards%d_%d" % (block, index)
                if group:
                    arrivals = ["%s%d" % (flags[block], mask) for mask in group if mask]
                    action = functools.partial(add_shards, block, group, index == 0)
                else:
                    arrivals = ["all_" + flags[block]]
                    action = functools.partial(whole_project, block)
                plan.task(name, 0.25 * len(group) + 0.47, before[block] + arrivals, action)
                before[block] = [name]
            name = "attend%d" % block
            plan.task(name, 2.95, before[block] + ["tangent"], functools.partial(attend, block))
        name = "probe%d" % pair_of[0]
        needs = ["attend%d" % block for block in pair_of] + sign_names
        plan.task(name, 3.8, needs, functools.partial(probe, pair_of))
    needs = ["shards1_%d" % (len(groups) - 1)]
    plan.task("turn", 1.7, needs, transpose_normed)
    needs = ["probe0", "probe2", "all_fd", "all_ed"]
    plan.task("forward1", 3.0, needs, functools.partial(forward, 1))
    plan.task("forward0", 3.0, ["forward1", "out1_0"], functools.partial(forward, 0))
    far_first = bits[2:] + bits[:2]
    out_order = sorted(range(shards), key=lambda mask: [-(mask & bit) for bit in far_first])
    value_order = sorted(range(shards), key=lambda mask: [-(mask & bit) for bit in bits])
    terms = []
    for at in range(0, shards, 2):
        for half in (1, 0):
            action = functools.partial(out_term, out_order[at : at + 2], half)
            terms.append(("out%d_%d" % (half, at), 1.1, ("forward%d" % half,), action))
    chain = []
    for group, block_pair in ((1, (2, 3)), (0, (0, 1))):
        for block in block_pair:
            needs = ("forward0", "forward1")
            chain.append(("back%d" % block, 1.5, needs, functools.partial(back_context, block)))
            action = functools.partial(spread_back, block)
            chain.append(("spread%d" % block, 0.5, ("back%d" % block,), action))
        needs = ["turn"] + ["spread%d" % block for block in block_pair]
        for at in range(0, shards, 2):
            action = functools.partial(value_term, value_order[at : at + 2], group)
            chain.append(("value%d_%d" % (group, at), 0.4, needs, action))
    merged = terms[:FIRST_TERMS]
    rest = terms[FIRST_TERMS:]
    while rest or chain:
        merged += chain[:CHAIN_STEP]
        merged += rest[:TERM_STEP]
        chain, rest = chain[CHAIN_STEP:], rest[TERM_STEP:]
    for entry in merged:
        plan.task(*entry)
    plan.run()
    drain(list(sent))


def body(hidden, norm_gain, query_weight, key_weight, value_weight, output_weight, probe_seed):
    tokens, width = hidden.shape
    query_width, key_width = query_weight.shape[1], key_weight.shape[1]
    probes, shards = lax.axis_size("probe"), lax.axis_size("fsdp")
    sizes = (shards, tokens, width, query_width, key_width, probes)
    assert probes == 4 and key_width == probes * HEAD_DIM and width == query_width
    scratch, streams, slots = layout(*sizes)
    cosine, sine = turn_tables()
    vmem = pl.BlockSpec(memory_space=pltpu.VMEM)
    anywhere = pl.BlockSpec(memory_space=pl.ANY)
    rows = width // shards
    return pl.pallas_call(
        functools.partial(kernel, sizes, list(scratch), streams, slots),
        in_specs=[pl.BlockSpec(memory_space=pltpu.SMEM)] + [vmem] * 3 + [anywhere] * 5,
        out_specs=[vmem, vmem],
        out_shape=[
            jax.ShapeDtypeStruct((rows, key_width // probes), F32),
            jax.ShapeDtypeStruct((rows, width // probes), F32),
        ],
        scratch_shapes=list(scratch.values()),
        compiler_params=pltpu.CompilerParams(
            collective_id=0, has_side_effects=True, vmem_limit_bytes=67043328
        ),
    )(
        probe_seed,
        norm_gain.reshape(1, width),
        jnp.asarray(cosine),
        jnp.asarray(sine),
        hidden,
        query_weight,
        key_weight,
        value_weight,
        output_weight,
    )


def solution(mesh):
    return jax.shard_map(
        body,
        mesh=mesh,
        in_specs=(
            P(("probe", "fsdp"), None),
            P(),
            P("fsdp", None),
            P("fsdp", None),
            P("fsdp", None),
            P("fsdp", None),
            P("probe"),
        ),
        out_specs=(P("fsdp", "probe"), P("fsdp", "probe")),
        check_vma=False,
    )
```
